32 devices in a mesh: fsdp: 8 (over y, x, core), tp: 4 (over z).
Axes of the slice: x: 2, y: 2, z: 4, core: 2. Of those that a mesh axis runs over, the one named last changes fastest.
Arguments:
- inputs: bfloat16 [16, 1024, 1536], P('fsdp', 'tp'), may hold values from -6 to 6
- teacher: bfloat16 [16, 1024, 1536], P('fsdp', 'tp'), may hold values from -6 to 6
- seq_lengths: int32 [16], P('fsdp'), may hold values from 256 to 1024, as said below
- first_gain: float32 [1536], replicated, may hold values from 0.5 to 1.5
- branch_weight: bfloat16 [1536, 2048], P('fsdp', 'tp'), may hold values from -0.15625 to 0.15625
- branch_bias: float32 [2048], P('tp'), may hold values from -3 to 3
- gate_weight: bfloat16 [1536, 2048], P('fsdp', 'tp'), may hold values from -0.15625 to 0.15625
- gate_bias: float32 [2048], P('tp'), may hold values from -3 to 3
- conv_weight: float32 [4, 2048], P(None, 'tp'), may hold values from -3 to 3
- conv_bias: float32 [2048], P('tp'), may hold values from -2 to 2
- rate_weight: bfloat16 [8, 256, 256], P('tp', 'fsdp'), may hold values from -0.375 to 0.375
- rate_bias: float32 [2048], P('tp'), may hold values from -4 to 4
- inlet_weight: bfloat16 [8, 256, 256], P('tp', 'fsdp'), may hold values from -0.375 to 0.375
- inlet_bias: float32 [2048], P('tp'), may hold values from -4 to 4
- decay_param: float32 [2048], P('tp'), may hold values from 3 to 11
- out_weight: bfloat16 [2048, 1536], P('tp', 'fsdp'), may hold values from -0.375 to 0.375
- second_gain: float32 [1536], replicated, may hold values from 0.5 to 1.5
- geglu_gate: bfloat16 [1536, 4608], P('fsdp', 'tp'), may hold values from -0.15625 to 0.15625
- geglu_up: bfloat16 [1536, 4608], P('fsdp', 'tp'), may hold values from -0.15625 to 0.15625
- geglu_down: bfloat16 [4608, 1536], P('tp', 'fsdp'), may hold values from -0.125 to 0.125
Outputs:
- block_out: bfloat16 [16, 1024, 1536], P('fsdp', 'tp')
- loss_value: float32 [], replicated
- input_grad: float32 [16, 1024, 1536], P('fsdp', 'tp')
- first_gain_grad: float32 [1536], replicated
- branch_weight_grad: float32 [1536, 2048], P('fsdp', 'tp')
- branch_bias_grad: float32 [2048], P('tp')
- gate_weight_grad: float32 [1536, 2048], P('fsdp', 'tp')
- gate_bias_grad: float32 [2048], P('tp')
- conv_weight_grad: float32 [4, 2048], P(None, 'tp')
- conv_bias_grad: float32 [2048], P('tp')
- rate_weight_grad: float32 [8, 256, 256], P('tp', 'fsdp')
- rate_bias_grad: float32 [2048], P('tp')
- inlet_weight_grad: float32 [8, 256, 256], P('tp', 'fsdp')
- inlet_bias_grad: float32 [2048], P('tp')
- decay_param_grad: float32 [2048], P('tp')
- out_weight_grad: float32 [2048, 1536], P('tp', 'fsdp')
- second_gain_grad: float32 [1536], replicated
- geglu_gate_grad: float32 [1536, 4608], P('fsdp', 'tp')
- geglu_up_grad: float32 [1536, 4608], P('fsdp', 'tp')
- geglu_down_grad: float32 [4608, 1536], P('tp', 'fsdp')
The draws below stay inside these ranges and needn't reach their ends.
Inputs may be any that keep to these rules, and one draw needn't show every extreme that they name: Position p of sequence s is valid where p < seq_lengths[s]; positions from seq_lengths[s] to 1023 are padding.
All inputs are finite; a program needn't handle non-finite values.
Results may differ from the reference program's by a relative error of at most 0.006.
Values may be sent and summed in bfloat16 or wider, within the bound.
No kernel may reach another device: no remote copies, remote signals or barrier semaphores. Data moves between devices by JAX's collectives and lax.ppermute only.
A program may use at most 256 MiB of HBM per device.

```python
import jax
import jax.numpy as jnp
from jax import lax

D = 1536
R = 2048
FF = 4608
GB = 256
CONV = 4
LENGTH = 1024
MIN_LEN = 256
SEQ_DEV = 2
SEQS = 16
NB = 8


def draw_seq_lengths(key, part):
    groups = SEQS // SEQ_DEV
    order = jnp.arange(SEQS, dtype=jnp.int32)
    owner = order // SEQ_DEV
    base = MIN_LEN + (LENGTH - MIN_LEN) * owner // max(groups - 1, 1)
    spare = (base - MIN_LEN) // 2 + 1
    jitter = jax.random.randint(jax.random.fold_in(key, 11), (SEQS,), 0, spare)
    chosen = jax.random.randint(jax.random.fold_in(key, 12), (), 1, SEQS)
    return jnp.where(order == chosen, LENGTH, base - jitter).astype(jnp.int32)


def raised(array, rng, source, target, blocks, factor):
    def block_of(axis_at):
        return (jnp.arange(array.shape[axis_at]) // (array.shape[axis_at] // blocks)).reshape((-1,) + (1,) * (array.ndim - 1 - axis_at))

    first = jax.random.permutation(rng, blocks)[block_of(target)]
    second = (block_of(target) + blocks // 2) % blocks
    return jnp.where((block_of(source) == first) | (block_of(source) == second), factor * array, array)


def levels(own_key, extent, split, smallest, high):
    level = 1.0
    for axis_at, blocks in split:
        steps = jax.random.uniform(jax.random.fold_in(jax.random.fold_in(own_key, 6), axis_at), (blocks,), jnp.float32, smallest / len(split), high / len(split))
        level = level * jnp.repeat(jnp.exp(steps), extent[axis_at] // blocks).reshape((-1,) + (1,) * (len(extent) - 1 - axis_at))
    return level


def noise(key, dims, deviation, reach, shards=(), kind=jnp.bfloat16):
    loudness = levels(key, dims, shards, -0.22, 0.18) if shards else 1.0
    drawn = jax.random.normal(key, dims, jnp.float32) * deviation * loudness
    return jnp.minimum(jnp.maximum(drawn, -reach), reach).astype(kind)


def gaussian_with(stream_key, shape, scale, limit, pieces, heavy, held_as=jnp.bfloat16):
    array = scale * jax.random.normal(stream_key, shape, jnp.float32)
    if pieces:
        array = array * levels(stream_key, shape, pieces, -0.22, 0.18)
    return jnp.clip(raised(array, jax.random.fold_in(stream_key, 3), *heavy), -limit, limit).astype(held_as)


def setup_inputs(seed: int = 0) -> dict:
    splits = jax.random.split(jax.random.key(seed), 21)
    return {
        "inputs": noise(splits[0], (SEQS, LENGTH, D), 1.0, 6.0, ((0, 8), (1, 4))),
        "teacher": gaussian_with(splits[1], (SEQS, LENGTH, D), 1.0, 6.0, ((0, 8), (1, 4)), (0, 2, 8, 2.0)),
        "seq_lengths": draw_seq_lengths(jax.random.fold_in(splits[20], 71), 0),
        "first_gain": jnp.clip(1.0 + 0.1 * jax.random.normal(splits[3], (D,), jnp.float32), 0.5, 1.5),
        "branch_weight": noise(splits[4], (D, R), D ** -0.5, 0.15625, ((0, 8), (1, 4))),
        "branch_bias": noise(splits[5], (R,), 0.5, 3.0, ((0, 4),), jnp.float32),
        "gate_weight": noise(splits[6], (D, R), D ** -0.5, 0.15625, ((0, 8), (1, 4))),
        "gate_bias": noise(splits[7], (R,), 0.5, 3.0, ((0, 4),), jnp.float32),
        "conv_weight": noise(splits[8], (CONV, R), 0.5, 3.0, ((1, 4),), jnp.float32),
        "conv_bias": noise(splits[9], (R,), 0.3, 2.0, ((0, 4),), jnp.float32),
        "rate_weight": noise(splits[10], (NB, GB, GB), GB ** -0.5, 0.375, ((0, 4), (1, 8))),
        "rate_bias": noise(splits[11], (R,), 1.0, 4.0, ((0, 4),), jnp.float32),
        "inlet_weight": noise(splits[12], (NB, GB, GB), GB ** -0.5, 0.375, ((0, 4), (1, 8))),
        "inlet_bias": noise(splits[13], (R,), 1.0, 4.0, ((0, 4),), jnp.float32),
        "decay_param": jnp.clip(3.0 + 8.0 * jax.random.uniform(splits[14], (R,), jnp.float32) ** levels(splits[14], (R,), ((0, 4),), -0.2, 0.2), 3.0, 11.0),
        "out_weight": noise(splits[15], (R, D), (R // 8) ** -0.5, 0.375, ((0, 4), (1, 8))),
        "second_gain": jnp.clip(1.0 + 0.1 * jax.random.normal(splits[16], (D,), jnp.float32), 0.5, 1.5),
        "geglu_gate": noise(splits[17], (D, FF), D ** -0.5, 0.15625, ((0, 8), (1, 4))),
        "geglu_up": noise(splits[18], (D, FF), D ** -0.5, 0.15625, ((0, 8), (1, 4))),
        "geglu_down": noise(splits[19], (FF, D), (FF // 2) ** -0.5, 0.125, ((0, 4), (1, 8))),
    }


EPS = 1e-06
DECAY_SCALE = 8.0
PRECISE = lax.Precision.HIGHEST

@jax.custom_vjp
def low(v):
    return lax.optimization_barrier(v.astype(jnp.bfloat16)).astype(jnp.float32)

@jax.custom_vjp
def low_back(v):
    return v

def low_keep(v):
    return (low(v), None)

def low_pass(kept, grad):
    return (grad,)

def back_keep(v):
    return (v, None)

def back_low(kept, grad):
    return (low(grad),)
low.defvjp(low_keep, low_pass)
low_back.defvjp(back_keep, back_low)

def rms_norm(values, gain_vec):
    inv_rms = lax.rsqrt(lax.optimization_barrier(jnp.mean(values * values, axis=-1, keepdims=True)) + EPS)
    return values * inv_rms * gain_vec

def causal_conv(branch, kernel, offset_bias):
    tap_count = kernel.shape[0]
    seq_len = branch.shape[1]
    padded = jnp.pad(branch, ((0, 0), (tap_count - 1, 0), (0, 0)))
    running = jnp.zeros_like(branch) + offset_bias
    for tap_index in range(tap_count):
        begin = tap_count - 1 - tap_index
        running = running + kernel[tap_index] * padded[:, begin:begin + seq_len]
    return running

def linear_scan(decay_rate, source):

    def combine(earlier, later):
        return (earlier[0] * later[0], later[0] * earlier[1] + later[1])
    return lax.associative_scan(combine, (decay_rate, source), axis=1)[1]

def lru_gates(rate_pre, inlet_pre, decay_param, conv_out):
    rate_gate = jax.nn.sigmoid(rate_pre)
    inlet_gate = jax.nn.sigmoid(inlet_pre)
    log_decay = -DECAY_SCALE * rate_gate * jax.nn.softplus(-decay_param)
    decay_rate = jnp.exp(log_decay)
    normaliser = jnp.sqrt(-jnp.expm1(2.0 * log_decay))
    return (decay_rate, normaliser * inlet_gate * conv_out)

def dense(values, matrix):
    return jnp.einsum('slk,kn->sln', values, matrix, precision=PRECISE)

def blockwise(values, block_weight):
    seqs_here, seq_len, channels = values.shape
    count_blocks = block_weight.shape[0]
    split_values = values.reshape(seqs_here, seq_len, count_blocks, channels // count_blocks)
    mapped = jnp.einsum('slbi,bij->slbj', split_values, block_weight, precision=PRECISE)
    return mapped.reshape(seqs_here, seq_len, channels)

def group_forward(inputs, teacher, valid_mask, params):
    first_gain, branch_weight, branch_bias, gate_weight, gate_bias, conv_weight, conv_bias, rate_weight, rate_bias, inlet_weight, inlet_bias, decay_param, out_weight, second_gain, geglu_gate, geglu_up, geglu_down = params
    normed = low(rms_norm(inputs, first_gain))
    branch = low_back(dense(normed, branch_weight) + branch_bias)
    gate_pre = low_back(dense(normed, gate_weight) + gate_bias)
    conv_out = low(causal_conv(branch, conv_weight, conv_bias))
    rate_pre = low_back(blockwise(conv_out, rate_weight) + rate_bias)
    inlet_pre = low_back(blockwise(conv_out, inlet_weight) + inlet_bias)
    decay_rate, source = lru_gates(rate_pre, inlet_pre, decay_param, conv_out)
    state = linear_scan(decay_rate, source)
    mixed = low(state * jax.nn.gelu(gate_pre))
    middle = inputs + low_back(dense(mixed, out_weight))
    second = low(rms_norm(middle, second_gain))
    ff_gate = low_back(dense(second, geglu_gate))
    ff_up = low_back(dense(second, geglu_up))
    ff_hidden = low(jax.nn.gelu(ff_gate) * ff_up)
    final = middle + low_back(dense(ff_hidden, geglu_down))
    mismatch = final - teacher
    return (final, jnp.sum(valid_mask[..., None] * mismatch * mismatch))

def reference(inputs, teacher, seq_lengths, first_gain, branch_weight, branch_bias, gate_weight, gate_bias, conv_weight, conv_bias, rate_weight, rate_bias, inlet_weight, inlet_bias, decay_param, out_weight, second_gain, geglu_gate, geglu_up, geglu_down):
    params = tuple((item.astype(jnp.float32) for item in (first_gain, branch_weight, branch_bias, gate_weight, gate_bias, conv_weight, conv_bias, rate_weight, rate_bias, inlet_weight, inlet_bias, decay_param, out_weight, second_gain, geglu_gate, geglu_up, geglu_down)))
    activations = inputs.astype(jnp.float32)
    targets = teacher.astype(jnp.float32)
    groups = SEQS // SEQ_DEV
    positions = jnp.arange(LENGTH, dtype=jnp.int32)
    valid_mask = (positions[None, :] < seq_lengths[:, None]).astype(jnp.float32)
    count = jnp.sum(seq_lengths.astype(jnp.float32))
    checked = jax.checkpoint(group_forward)

    def forward(acts, weights):

        def step(running, item):
            final, part = checked(item[0], item[1], item[2], weights)
            return (running + part, final)
        shaped = (acts.reshape(groups, SEQ_DEV, LENGTH, D), targets.reshape(groups, SEQ_DEV, LENGTH, D), valid_mask.reshape(groups, SEQ_DEV, LENGTH))
        total, finals = lax.scan(step, jnp.zeros((), jnp.float32), shaped)
        return (finals.reshape(SEQS, LENGTH, D), total / (D * count))
    (finals, loss_value), pullback = jax.vjp(forward, activations, params)
    input_grad, grads = pullback((jnp.zeros_like(finals), jnp.asarray(SEQS * LENGTH * D / 2, jnp.float32)))
    return (finals.astype(jnp.bfloat16), loss_value, input_grad, grads[0], grads[1], grads[2], grads[3], grads[4], grads[5], grads[6], grads[7], grads[8], grads[9], grads[10], grads[11], grads[12], grads[13], grads[14], grads[15], grads[16])
```

```python
import functools

import jax
import jax.numpy as jnp
from jax import lax
from jax.experimental import pallas as pl
from jax.experimental.pallas import tpu as pltpu
from jax.sharding import PartitionSpec as P

EPS = 1e-06
DECAY_SCALE = 8.0
BF = jnp.bfloat16
F32 = jnp.float32
STEP = 16
GELU_A = 0.7978845608028654
GELU_B = 0.044715


def swap(values, axis_name, bit):
    size = lax.axis_size(axis_name)
    return lax.ppermute(values, axis_name, [(i, i ^ bit) for i in range(size)])


def bits_of(count):
    return [1 << b for b in range(count.bit_length() - 1)]


def in_core_order(mine, other, core, axis):
    first = jnp.where(core == 0, mine, other)
    second = jnp.where(core == 0, other, mine)
    return jnp.concatenate([first, second], axis=axis)


def pick_half(values, which, axis):
    low, high = jnp.split(values, 2, axis=axis)
    return jnp.where(which == 0, low, high)


def xor_blocks(values, axis, count, index):
    blocks = jnp.split(values, count, axis=axis)
    for bit in bits_of(count):
        flipped = (index & bit) != 0
        blocks = [jnp.where(flipped, blocks[j ^ bit], blocks[j]) for j in range(count)]
    return jnp.concatenate(blocks, axis=axis)


def lane_blocks(values, count, wanted):
    width = values.shape[1] // count
    runs, start = [], 0
    while start < len(wanted):
        stop = start + 1
        while stop < len(wanted) and wanted[stop] == wanted[stop - 1] + 1:
            stop += 1
        runs.append(values[:, wanted[start] * width : (wanted[stop - 1] + 1) * width])
        start = stop
    return runs[0] if len(runs) == 1 else jnp.concatenate(runs, axis=1)


def gather_matrix(unit, order):
    held = [0]
    for kind, bit in order:
        other = swap(unit, *((("tp", bit)) if kind == "z" else ("fsdp", 2 * bit)))
        if kind == "z":
            unit = jnp.concatenate([unit, other], axis=0)
            continue
        width = unit.shape[1] // len(held)
        parts = {j: unit[:, k * width : (k + 1) * width] for k, j in enumerate(held)}
        parts |= {j ^ bit: other[:, k * width : (k + 1) * width] for k, j in enumerate(held)}
        held = sorted(parts)
        unit = jnp.concatenate([parts[j] for j in held], axis=1)
    return unit


def scatter_matrix(total, order, chips):
    held = list(range(chips))
    for step, (kind, bit) in enumerate(reversed(order)):
        if kind == "z":
            keep, send = jnp.split(total, 2, axis=0)
            got = swap(send, "tp", bit)
        else:
            at = {j: k for k, j in enumerate(held)}
            count = len(held)
            send = lane_blocks(total, count, [at[j] for j in held if j & bit])
            keep = lane_blocks(total, count, [at[j] for j in held if not j & bit])
            held = [j for j in held if not j & bit]
            got = swap(send, "fsdp", 2 * bit)
        total = keep.astype(F32) + got.astype(F32)
        if step < len(order) - 1:
            total = total.astype(BF)
    return total


def minus_expm1(y):
    series = 1.0 + y * (1.0 / 7.0)
    for n in (6.0, 5.0, 4.0, 3.0, 2.0):
        series = 1.0 + y * (1.0 / n) * series
    return jnp.where(y > -0.35, -y * series, 1.0 - jnp.exp(y))


def sigmoid(v):
    return 0.5 * jnp.tanh(0.5 * v) + 0.5


def rows_iota(width):
    return lax.broadcasted_iota(jnp.int32, (8, width), 0)


def forward_kernel(
    branch,
    halo,
    conv_w,
    vectors,
    rate_w,
    inlet_w,
    conv_out,
    decay_out,
    local_out,
    prod_out,
    ext,
    rate_s,
    inlet_s,
):
    length, width = branch.shape[1:]
    ext[0:8] = halo[0]
    ext[8:] = branch[0]
    taps = conv_w.shape[0]

    def conv_step(i, carry):
        at = pl.multiple_of(i * STEP, STEP)
        window = ext[pl.ds(at, STEP + 8), :]
        total = jnp.broadcast_to(vectors[0:1, :], (STEP, width))
        for k in range(taps):
            total = total + conv_w[k : k + 1, :] * window[8 - k : 8 - k + STEP]
        conv_out[0, pl.ds(at, STEP), :] = total.astype(BF)
        return carry

    lax.fori_loop(0, length // STEP, conv_step, 0)
    mixed = conv_out[0]
    rate_s[...] = jnp.dot(mixed, rate_w[0], preferred_element_type=F32) + vectors[1:2, :]
    inlet_s[...] = jnp.dot(mixed, inlet_w[0], preferred_element_type=F32) + vectors[2:3, :]
    row = rows_iota(width)

    def scan_step(i, carry):
        at = pl.multiple_of(i * STEP, STEP)
        rows = pl.ds(at, STEP)
        rate = sigmoid(rate_s[rows, :])
        log_decay = (-DECAY_SCALE * rate) * vectors[3:4, :]
        decay = jnp.exp(log_decay)
        scale = jnp.sqrt(minus_expm1(2.0 * log_decay))
        source = scale * sigmoid(inlet_s[rows, :]) * conv_out[0, rows, :].astype(F32)
        decay_out[0, rows, :] = decay
        held, prod = carry
        for part in range(STEP // 8):
            a = decay[8 * part : 8 * part + 8]
            b = source[8 * part : 8 * part + 8]
            for k in (1, 2, 4):
                ok = row >= k
                b = jnp.where(ok, a * pltpu.roll(b, k, 0) + b, b)
                a = jnp.where(ok, a * pltpu.roll(a, k, 0), a)
            b = b + a * held
            a = a * prod
            here = pl.ds(at + 8 * part, 8)
            local_out[0, here, :] = b
            prod_out[0, here, :] = a
            held, prod = b[7:8], a[7:8]
        return held, prod

    lax.fori_loop(
        0,
        length // STEP,
        scan_step,
        (jnp.zeros((1, width), F32), jnp.ones((1, width), F32)),
    )


def block_spec(shape, index):
    return pl.BlockSpec(shape, index)


def run_forward(branch, halo, conv_w, vectors, rate_w, inlet_w):
    seqs, length, channels = branch.shape
    width = rate_w.shape[1]
    wide = pl.BlockSpec((1, length, width), lambda j, s: (s, 0, j))
    gate = pl.BlockSpec((1, width, width), lambda j, s: (j, 0, 0))
    full = lambda dt: jax.ShapeDtypeStruct(branch.shape, dt)
    return pl.pallas_call(
        forward_kernel,
        grid=(channels // width, seqs),
        in_specs=[
            wide,
            pl.BlockSpec((1, 8, width), lambda j, s: (s, 0, j)),
            pl.BlockSpec((conv_w.shape[0], width), lambda j, s: (0, j)),
            pl.BlockSpec((vectors.shape[0], width), lambda j, s: (0, j)),
            gate,
            gate,
        ],
        out_specs=[wide] * 4,
        out_shape=[full(BF), full(F32), full(F32), full(F32)],
        scratch_shapes=[
            pltpu.VMEM((length + 8, width), F32),
            pltpu.VMEM((length, width), F32),
            pltpu.VMEM((length, width), F32),
        ],
        cost_estimate=pl.CostEstimate(
            flops=60 * branch.size + 4 * branch.size * width,
            bytes_accessed=20 * branch.size,
            transcendentals=4 * branch.size,
        ),
        name="forward_scan",
    )(branch, halo, conv_w, vectors, rate_w, inlet_w)


def gelu_parts(x):
    square = x * x
    t = jnp.tanh(GELU_A * x * (1.0 + GELU_B * square))
    half = 0.5 * (1.0 + t)
    slope = half + 0.5 * x * (1.0 - t * t) * (GELU_A * (1.0 + 3.0 * GELU_B * square))
    return x * half, slope


def backward_scan_kernel(d_mixed, gate_pre, state, decay, d_gate, local_out, prod_out):
    length, width = state.shape[1:]
    row = rows_iota(width)

    def step(n, carry):
        at = pl.multiple_of(length - STEP - n * STEP, STEP)
        rows = pl.ds(at, STEP)
        dm = d_mixed[0, rows, :].astype(F32)
        act, slope = gelu_parts(gate_pre[0, rows, :])
        d_gate[0, rows, :] = (dm * state[0, rows, :] * slope).astype(BF)
        d_state = dm * act
        all_decay = decay[0, rows, :]
        held, prod, above = carry
        for part in reversed(range(STEP // 8)):
            plain = all_decay[8 * part : 8 * part + 8]
            a = jnp.where(row == 7, above, pltpu.roll(plain, 7, 0))
            b = d_state[8 * part : 8 * part + 8]
            for k in (1, 2, 4):
                ok = row < 8 - k
                b = jnp.where(ok, a * pltpu.roll(b, 8 - k, 0) + b, b)
                a = jnp.where(ok, a * pltpu.roll(a, 8 - k, 0), a)
            b = b + a * held
            a = a * prod
            here = pl.ds(at + 8 * part, 8)
            local_out[0, here, :] = b
            prod_out[0, here, :] = a
            held, prod, above = b[0:1], a[0:1], plain[0:1]
        return held, prod, above

    one = jnp.ones((1, width), F32)
    lax.fori_loop(0, length // STEP, step, (jnp.zeros((1, width), F32), one, one))


def run_backward_scan(d_mixed, gate_pre, state, decay, width):
    seqs, length, channels = state.shape
    wide = pl.BlockSpec((1, length, width), lambda j, s: (s, 0, j))
    full = lambda dt: jax.ShapeDtypeStruct(state.shape, dt)
    return pl.pallas_call(
        backward_scan_kernel,
        grid=(channels // width, seqs),
        in_specs=[wide] * 4,
        out_specs=[wide] * 3,
        out_shape=[full(BF), full(F32), full(F32)],
        cost_estimate=pl.CostEstimate(
            flops=60 * state.size, bytes_accessed=24 * state.size, transcendentals=state.size
        ),
        name="backward_scan",
    )(d_mixed, gate_pre, state, decay)


def backward_gates_kernel(
    local_c,
    prod_c,
    carry_in,
    state,
    state_in,
    conv_out,
    branch,
    halo,
    conv_w,
    vectors,
    rate_w,
    inlet_w,
    d_branch,
    head_out,
    tail_out,
    g_rate,
    g_inlet,
    sums,
    branch_x,
    state_x,
    rate_s,
    inlet_s,
    d_rate_s,
    d_inlet_s,
    d_conv_x,
):
    length, width = state.shape[1:]
    taps = conv_w.shape[0]
    seq = pl.program_id(1)
    branch_x[0:8] = halo[0]
    branch_x[8:] = branch[0]
    state_x[0:8] = jnp.broadcast_to(state_in[0], (8, width))
    state_x[8:] = state[0]
    mixed = conv_out[0]
    rate_s[...] = jnp.dot(mixed, rate_w[0], preferred_element_type=F32) + vectors[1:2, :]
    inlet_s[...] = jnp.dot(mixed, inlet_w[0], preferred_element_type=F32) + vectors[2:3, :]
    zero = jnp.zeros((8, width), F32)

    @pl.when(seq == 0)
    def _():
        g_rate[...] = jnp.zeros_like(g_rate)
        g_inlet[...] = jnp.zeros_like(g_inlet)
        sums[...] = jnp.zeros_like(sums)

    def fold(v):
        total = v[0:8]
        for part in range(1, STEP // 8):
            total = total + v[8 * part : 8 * part + 8]
        return total

    def gate_step(i, carry):
        s_decay, s_rate, s_inlet = carry
        at = pl.multiple_of(i * STEP, STEP)
        rows = pl.ds(at, STEP)
        rate = sigmoid(rate_s[rows, :])
        inlet = sigmoid(inlet_s[rows, :])
        log_decay = (-DECAY_SCALE * rate) * vectors[3:4, :]
        decay = jnp.exp(log_decay)
        scale = jnp.sqrt(minus_expm1(2.0 * log_decay))
        conv = conv_out[0, rows, :].astype(F32)
        cot = local_c[0, rows, :] + prod_c[0, rows, :] * carry_in[0]
        before = state_x[pl.ds(at, STEP + 8), :][7 : 7 + STEP]
        gated = cot * inlet
        d_log = cot * before * decay - gated * conv * (decay * decay) / scale
        weighted = d_log * rate
        d_rate = (weighted * (1.0 - rate) * (-DECAY_SCALE * vectors[3:4, :])).astype(BF)
        d_inlet = (gated * scale * conv * (1.0 - inlet)).astype(BF)
        d_rate_s[rows, :] = d_rate
        d_inlet_s[rows, :] = d_inlet
        d_conv_x[rows, :] = gated * scale
        return (
            s_decay + fold(weighted),
            s_rate + fold(d_rate.astype(F32)),
            s_inlet + fold(d_inlet.astype(F32)),
        )

    s_decay, s_rate, s_inlet = lax.fori_loop(0, length // STEP, gate_step, (zero, zero, zero))
    d_rate, d_inlet = d_rate_s[...], d_inlet_s[...]
    over_rows = (((0,), (0,)), ((), ()))
    transposed = (((1,), (1,)), ((), ()))
    g_rate[0] += lax.dot_general(mixed, d_rate, over_rows, preferred_element_type=F32)
    g_inlet[0] += lax.dot_general(mixed, d_inlet, over_rows, preferred_element_type=F32)
    d_conv_x[0:length] += lax.dot_general(
        d_rate, rate_w[0], transposed, preferred_element_type=F32
    ) + lax.dot_general(d_inlet, inlet_w[0], transposed, preferred_element_type=F32)
    d_conv_x[length:] = zero
    head_out[0] = d_conv_x[0:8]

    def conv_step(i, carry):
        at = pl.multiple_of(i * STEP, STEP)
        ahead = d_conv_x[pl.ds(at, STEP + 8), :]
        behind = branch_x[pl.ds(at, STEP + 8), :]
        here = ahead[0:STEP]
        total = conv_w[0:1, :] * here
        new = [carry[0] + fold(here)]
        for k in range(taps):
            if k:
                total = total + conv_w[k : k + 1, :] * ahead[k : k + STEP]
            new.append(carry[k + 1] + fold(here * behind[8 - k : 8 - k + STEP]))
        d_branch[0, pl.ds(at, STEP), :] = total.astype(BF)
        tail_out[0] = total[STEP - 8 : STEP]
        return tuple(new)

    found = lax.fori_loop(0, length // STEP, conv_step, (zero,) * (taps + 1))
    for k, total in enumerate((s_decay, s_rate, s_inlet, *found)):
        sums[k] += total


def run_backward_gates(
    local_c, prod_c, carry_in, state, state_in, conv_out, branch, halo, conv_w, vectors, rate_w, inlet_w
):
    seqs, length, channels = branch.shape
    width = rate_w.shape[1]
    taps = conv_w.shape[0]
    wide = pl.BlockSpec((1, length, width), lambda j, s: (s, 0, j))
    line = pl.BlockSpec((1, 1, width), lambda j, s: (s, 0, j))
    edge = pl.BlockSpec((1, 8, width), lambda j, s: (s, 0, j))
    gate = pl.BlockSpec((1, width, width), lambda j, s: (j, 0, 0))
    edge_shape = jax.ShapeDtypeStruct((seqs, 8, channels), F32)
    gate_shape = jax.ShapeDtypeStruct(rate_w.shape, F32)
    return pl.pallas_call(
        backward_gates_kernel,
        grid=(channels // width, seqs),
        in_specs=[
            wide,
            wide,
            line,
            wide,
            line,
            wide,
            wide,
            edge,
            pl.BlockSpec((taps, width), lambda j, s: (0, j)),
            pl.BlockSpec((vectors.shape[0], width), lambda j, s: (0, j)),
            gate,
            gate,
        ],
        out_specs=[
            wide,
            edge,
            edge,
            gate,
            gate,
            pl.BlockSpec((taps + 4, 8, width), lambda j, s: (0, 0, j)),
        ],
        out_shape=[
            jax.ShapeDtypeStruct(branch.shape, BF),
            edge_shape,
            edge_shape,
            gate_shape,
            gate_shape,
            jax.ShapeDtypeStruct((taps + 4, 8, channels), F32),
        ],
        scratch_shapes=[
            pltpu.VMEM((length + 8, width), F32),
            pltpu.VMEM((length + 8, width), F32),
            pltpu.VMEM((length, width), F32),
            pltpu.VMEM((length, width), F32),
            pltpu.VMEM((length, width), BF),
            pltpu.VMEM((length, width), BF),
            pltpu.VMEM((length + 8, width), F32),
        ],
        cost_estimate=pl.CostEstimate(
            flops=100 * branch.size + 12 * branch.size * width,
            bytes_accessed=22 * branch.size,
            transcendentals=5 * branch.size,
        ),
        name="backward_gates",
    )(local_c, prod_c, carry_in, state, state_in, conv_out, branch, halo, conv_w, vectors, rate_w, inlet_w)


def rms_norm(values, gain_vec):
    inv_rms = lax.rsqrt(jnp.mean(values * values, axis=-1, keepdims=True) + EPS)
    return values * inv_rms * gain_vec


def norm_back(values, gain_vec, cot):
    inv_rms = lax.rsqrt(jnp.mean(values * values, axis=-1, keepdims=True) + EPS)
    unit = values * inv_rms
    scaled = cot * gain_vec
    grad = inv_rms * (scaled - unit * jnp.mean(scaled * unit, axis=-1, keepdims=True))
    return grad, jnp.sum(cot * unit, axis=(0, 1))


def times(values, matrix, dtype=F32):
    return jnp.einsum("slk,kn->sln", values, matrix, preferred_element_type=dtype)


def times_t(values, matrix, dtype=F32):
    return jnp.einsum("sln,kn->slk", values, matrix, preferred_element_type=dtype)


def outer_sum(values, cotangent):
    return jnp.einsum("slk,sln->kn", values, cotangent, preferred_element_type=F32).astype(BF)


def shards(
    inputs,
    teacher,
    seq_lengths,
    first_gain,
    branch_weight,
    branch_bias,
    gate_weight,
    gate_bias,
    conv_weight,
    conv_bias,
    rate_weight,
    rate_bias,
    inlet_weight,
    inlet_bias,
    decay_param,
    out_weight,
    second_gain,
    geglu_gate,
    geglu_up,
    geglu_down,
):
    seq_dev, local_len, model_width = inputs.shape
    tp = lax.axis_size("tp")
    fsdp = lax.axis_size("fsdp")
    chips = fsdp // 2
    full_len = local_len * tp
    me = lax.axis_index("fsdp")
    z = lax.axis_index("tp")
    core = me & 1
    chip = me // 2
    width = rate_weight.shape[2]
    taps = conv_weight.shape[0]

    zs = [("z", b) for b in bits_of(tp)]
    ds = [("d", b) for b in bits_of(chips)]
    order_a = zs + ds
    order_b = zs + ds[::-1]
    order_mid_a = ds[:1] + zs + ds[1:]
    order_mid_b = ds[-1:] + zs + ds[:-1]

    def same_chip(values):
        return swap(values, "fsdp", 1)

    def both_rows(values):
        return in_core_order(values, same_chip(values), core, 0)

    def unit_of(matrix, channel_axis):
        mine = pick_half(matrix, core, channel_axis)
        other = same_chip(pick_half(matrix, 1 - core, channel_axis))
        if channel_axis == 1:
            mine, other = mine.T, other.T
        return in_core_order(mine, other, core, 1)

    x4 = both_rows(inputs)
    w_branch = gather_matrix(unit_of(branch_weight, 1), order_a)
    w_gate = gather_matrix(unit_of(gate_weight, 1), order_b)

    rows_chip = 2 * rate_weight.shape[1]
    pair = jnp.concatenate([rate_weight, inlet_weight], axis=1)
    pair_mine = pick_half(pair, core, 0)[0]
    pair_other = same_chip(pick_half(pair, 1 - core, 0)[0])
    pair_unit = in_core_order(
        pair_mine.reshape(2, -1, width), pair_other.reshape(2, -1, width), core, 1
    )

    def pack_pair(values):
        return values.reshape(values.shape[0], -1)

    held = pair_unit[None]
    for b in bits_of(tp):
        held = jnp.concatenate([held, swap(held, "tp", b)], axis=0)
    held = held[:, :, None]
    for b in bits_of(chips):
        held = jnp.concatenate([held, swap(held, "fsdp", 2 * b)], axis=2)
    held = xor_blocks(held, 2, chips, chip)
    held = held.reshape(tp, 2, chips * rows_chip, width)
    w_rate, w_inlet = held[:, 0], held[:, 1]

    w_out = gather_matrix(unit_of(out_weight, 0), order_mid_b)
    w_ffgate = gather_matrix(unit_of(geglu_gate, 1), order_a)
    w_ffup = gather_matrix(unit_of(geglu_up, 1), order_b)
    w_ffdown = gather_matrix(unit_of(geglu_down, 0), order_mid_a)

    def to_relative(values):
        return xor_blocks(values, values.ndim - 1, tp, z)

    local_vectors = jnp.concatenate(
        [
            conv_weight,
            jnp.stack([branch_bias, gate_bias, conv_bias, rate_bias, inlet_bias, decay_param]),
        ],
        axis=0,
    )
    held = pick_half(local_vectors, core, 1)
    for b in bits_of(tp):
        held = jnp.concatenate([held, swap(held, "tp", b)], axis=1)
    taps_w = held[:taps]
    b_branch, b_gate, b_conv, b_rate, b_inlet, decay_vec = (held[taps + k] for k in range(6))
    soft = jax.nn.softplus(-decay_vec)
    vectors = jnp.stack([b_conv, b_rate, b_inlet, soft])

    lengths4 = both_rows(seq_lengths)
    count = jnp.broadcast_to(jnp.sum(lengths4.astype(F32)), (8, 128))
    for b in bits_of(chips):
        count = count + swap(count, "fsdp", 2 * b)
    valid_total = count[0, 0]

    def to_chip(values):
        return xor_blocks(values, values.ndim - 1, chips, chip)

    gain1, gain2 = to_chip(first_gain), to_chip(second_gain)
    x4 = to_chip(x4)
    residual = x4.astype(F32)
    first_rows = rms_norm(residual, gain1).astype(BF)
    branch_pre = times_t(first_rows, w_branch) + b_branch
    gate_pre = times_t(first_rows, w_gate) + b_gate

    def along_z(values, shift):
        pairs = [(i, i + shift) for i in range(tp) if 0 <= i + shift < tp]
        return to_relative(lax.ppermute(to_relative(values), "tp", pairs))

    halo = jnp.pad(along_z(branch_pre[:, local_len - taps + 1 :], 1), ((0, 0), (8 - taps + 1, 0), (0, 0)))
    conv_out, decay_rate, local_state, prod_decay = run_forward(
        branch_pre, halo, taps_w, vectors, w_rate, w_inlet
    )
    ends = jnp.stack([prod_decay[:, -1], local_state[:, -1]])
    state_in = jnp.zeros_like(ends[0])
    for shift in reversed(range(1, tp)):
        got = along_z(ends, shift)
        state_in = got[1] + got[0] * state_in
    state_in = state_in[:, None]
    state = local_state + prod_decay * state_in
    mixed = (state * jax.nn.gelu(gate_pre)).astype(BF)

    def core_sum(term):
        return term.astype(F32) + same_chip(term).astype(F32)

    middle = residual + core_sum(times(mixed, w_out, BF))
    second_rows = rms_norm(middle, gain2).astype(BF)
    ff_gate = times_t(second_rows, w_ffgate)
    ff_up = times_t(second_rows, w_ffup)
    ff_hidden = (jax.nn.gelu(ff_gate) * ff_up).astype(BF)
    final = middle + core_sum(times(ff_hidden, w_ffdown, BF))

    positions = z * local_len + jnp.arange(local_len, dtype=jnp.int32)
    valid_mask = (positions[None, :] < lengths4[:, None]).astype(F32)[..., None]
    teacher4 = to_chip(both_rows(teacher)).astype(F32)
    mismatch = final - teacher4
    loss_part = jnp.sum(valid_mask * mismatch * mismatch)
    scaling = seq_dev * fsdp * full_len / valid_total
    out_cot = valid_mask * mismatch * scaling
    ff_cot = out_cot.astype(BF)

    g_ffdown = scatter_matrix(outer_sum(ff_hidden, ff_cot), order_mid_a, chips)
    d_hidden = times_t(ff_cot, w_ffdown)
    act, slope = gelu_parts(ff_gate)
    d_up = (d_hidden * act).astype(BF)
    d_ffgate = (d_hidden * ff_up * slope).astype(BF)
    g_ffgate = scatter_matrix(outer_sum(d_ffgate, second_rows), order_a, chips)
    g_ffup = scatter_matrix(outer_sum(d_up, second_rows), order_b, chips)
    d_second = core_sum((times(d_ffgate, w_ffgate) + times(d_up, w_ffup)).astype(BF))
    d_mid_norm, g_second = norm_back(middle, gain2, d_second)
    d_middle = out_cot + d_mid_norm
    mid_cot = d_middle.astype(BF)
    d_mixed = times_t(mid_cot, w_out)
    g_out = scatter_matrix(outer_sum(mixed, mid_cot), order_mid_b, chips)
    d_gate, local_c, prod_c = run_backward_scan(d_mixed, gate_pre, state, decay_rate, width)
    starts = jnp.stack([prod_c[:, 0], local_c[:, 0]]) * decay_rate[:, 0]
    carry_in = jnp.zeros_like(starts[0])
    for shift in reversed(range(1, tp)):
        got = along_z(starts, -shift)
        carry_in = got[1] + got[0] * carry_in
    g_gate = scatter_matrix(outer_sum(d_gate, first_rows), order_b, chips)
    d_branch, head, tail, g_rate, g_inlet, sums = run_backward_gates(
        local_c,
        prod_c,
        carry_in[:, None],
        state,
        state_in,
        conv_out,
        branch_pre,
        halo,
        taps_w,
        vectors,
        w_rate,
        w_inlet,
    )
    ahead = along_z(head[:, : taps - 1], -1)
    edge = tail[:, 8 - taps + 1 :]
    for k in range(1, taps):
        first = taps - 1 - k
        edge = edge.at[:, first:].add(taps_w[k] * ahead[:, :k])
    d_branch = lax.dynamic_update_slice(d_branch, edge.astype(BF), (0, local_len - taps + 1, 0))
    g_branch = scatter_matrix(outer_sum(d_branch, first_rows), order_a, chips)
    d_first_part = (times(d_branch, w_branch) + times(d_gate, w_gate)).astype(BF)

    def own(values):
        return pick_half(values, core, 0)

    d_first = own(d_first_part).astype(F32) + same_chip(pick_half(d_first_part, 1 - core, 0)).astype(F32)
    d_in_norm, g_first = norm_back(inputs_rel := own(residual), gain1, d_first)
    input_grad = to_chip(own(d_middle) + d_in_norm)
    block_out = to_chip(own(final).astype(BF))

    pair_g = jnp.stack([g_rate, g_inlet], axis=1).astype(BF)
    pair_g = pair_g.reshape(tp, 2, chips, rows_chip, width)
    pair_g = xor_blocks(pair_g, 2, chips, chip)
    for b in reversed(bits_of(chips)):
        keep, send = jnp.split(pair_g, 2, axis=2)
        pair_g = (keep.astype(F32) + swap(send, "fsdp", 2 * b).astype(F32)).astype(BF)
    for b in reversed(bits_of(tp)):
        keep, send = jnp.split(pair_g, 2, axis=0)
        pair_g = keep.astype(F32) + swap(send, "tp", b).astype(F32)
        if b > 1:
            pair_g = pair_g.astype(BF)
    pair_g = pair_g.reshape(2, rows_chip, width)
    pair_mine = pick_half(pair_g, core, 1)
    pair_other = same_chip(pick_half(pair_g, 1 - core, 1))
    pair_g = in_core_order(pair_mine[None], pair_other[None], core, 0)

    def to_own(grad, channel_axis):
        mine = pick_half(grad, core, 1)
        other = same_chip(pick_half(grad, 1 - core, 1))
        whole = in_core_order(mine, other, core, 0)
        return whole.T if channel_axis == 1 else whole

    sums = jnp.sum(sums, axis=1)
    small = jnp.concatenate(
        [
            jnp.stack(
                [
                    jnp.sum(d_branch.astype(F32), axis=(0, 1)),
                    jnp.sum(d_gate.astype(F32), axis=(0, 1)),
                    sums[0] * (DECAY_SCALE * jax.nn.sigmoid(-decay_vec)),
                ]
            ),
            sums[1:],
        ],
        axis=0,
    )
    for b in bits_of(chips):
        small = small + swap(small, "fsdp", 2 * b)
    for b in reversed(bits_of(tp)):
        keep, send = jnp.split(small, 2, axis=1)
        small = keep + swap(send, "tp", b)
    small = in_core_order(small, same_chip(small), core, 1)
    stats = jnp.stack(
        [
            jnp.broadcast_to(0.5 * loss_part, (model_width,)),
            to_chip(g_first),
            to_chip(0.5 * g_second),
        ]
    )
    for b in bits_of(fsdp):
        stats = stats + swap(stats, "fsdp", b)
    for b in bits_of(tp):
        stats = stats + swap(stats, "tp", b)
    loss_value = stats[0, 0] / (model_width * valid_total)
    return (
        block_out,
        loss_value,
        input_grad,
        stats[1],
        to_own(g_branch, 1),
        small[0],
        to_own(g_gate, 1),
        small[1],
        small[6:],
        small[5],
        pair_g[:, 0],
        small[3],
        pair_g[:, 1],
        small[4],
        small[2],
        to_own(g_out, 0),
        stats[2],
        to_own(g_ffgate, 1),
        to_own(g_ffup, 1),
        to_own(g_ffdown, 0),
    )


def solution(mesh):
    rows = P("fsdp", "tp", None)
    by_column, by_row = P("fsdp", "tp"), P("tp", "fsdp")
    blocks = P("tp", "fsdp", None)
    channel = P("tp")
    return jax.shard_map(
        shards,
        mesh=mesh,
        in_specs=(
            rows,
            rows,
            P("fsdp"),
            P(),
            by_column,
            channel,
            by_column,
            channel,
            P(None, "tp"),
            channel,
            blocks,
            channel,
            blocks,
            channel,
            channel,
            by_row,
            P(),
            by_column,
            by_column,
            by_row,
        ),
        out_specs=(
            rows,
            P(),
            rows,
            P(),
            by_column,
            channel,
            by_column,
            channel,
            P(None, "tp"),
            channel,
            blocks,
            channel,
            blocks,
            channel,
            channel,
            by_row,
            P(),
            by_column,
            by_column,
            by_row,
        ),
        check_vma=False,
    )
```

```python
import functools

import jax
import jax.numpy as jnp
from jax import lax
from jax.experimental import pallas as pl
from jax.experimental.pallas import tpu as pltpu
from jax.sharding import PartitionSpec as P

EPS = 1e-06
DECAY_SCALE = 8.0
BF = jnp.bfloat16
F32 = jnp.float32
STEP = 16
GELU_A = 0.7978845608028654
GELU_B = 0.044715
TINY = pl.CostEstimate(flops=1, bytes_accessed=1, transcendentals=0)


def swap(values, axis_name, bit):
    size = lax.axis_size(axis_name)
    return lax.ppermute(values, axis_name, [(i, i ^ bit) for i in range(size)])


def bits_of(count):
    return [1 << b for b in range(count.bit_length() - 1)]


def in_core_order(mine, other, core, axis):
    first = jnp.where(core == 0, mine, other)
    second = jnp.where(core == 0, other, mine)
    return jnp.concatenate([first, second], axis=axis)


def pick_half(values, which, axis):
    low, high = jnp.split(values, 2, axis=axis)
    return jnp.where(which == 0, low, high)


def xor_blocks(values, axis, count, index):
    blocks = jnp.split(values, count, axis=axis)
    for bit in bits_of(count):
        flipped = (index & bit) != 0
        blocks = [jnp.where(flipped, blocks[j ^ bit], blocks[j]) for j in range(count)]
    return jnp.concatenate(blocks, axis=axis)


def lane_blocks(values, count, wanted):
    width = values.shape[1] // count
    runs, start = [], 0
    while start < len(wanted):
        stop = start + 1
        while stop < len(wanted) and wanted[stop] == wanted[stop - 1] + 1:
            stop += 1
        runs.append(values[:, wanted[start] * width : (wanted[stop - 1] + 1) * width])
        start = stop
    return runs[0] if len(runs) == 1 else jnp.concatenate(runs, axis=1)


def after(value, *others):
    return lax.optimization_barrier((value, *others))[0]


def spread(pieces, bits):
    for bit in bits:
        held = sorted(pieces)
        if len(held) <= 2:
            got = {j ^ bit: swap(pieces[j], "fsdp", 2 * bit) for j in held}
        else:
            other = swap(jnp.concatenate([pieces[j] for j in held], axis=1), "fsdp", 2 * bit)
            width = pieces[held[0]].shape[1]
            got = {j ^ bit: other[:, k * width : (k + 1) * width] for k, j in enumerate(held)}
        pieces = pieces | got
    return pieces


def finish(pieces, ahead, bits):
    for bit in bits:
        got = {j ^ bit: swap(v, "fsdp", 2 * bit) for j, v in pieces.items() if j ^ bit not in ahead}
        pieces = pieces | ahead | got
        ahead = {}
    return pieces


def fence(*groups):
    return lax.optimization_barrier(groups)


def join_kernel(half, counts, *refs):
    out = refs[-1]
    first, second = refs[: counts[0]], refs[counts[0] : -1]

    def put(parts):
        width = parts[0].shape[1]
        for k, part in enumerate(parts):
            out[:, k * width : (k + 1) * width] = part[...]

    if not second:
        put(first)
        return
    pl.when(pl.program_id(0) < half)(lambda: put(first))
    pl.when(pl.program_id(0) >= half)(lambda: put(second))


def join(pieces, start=0, count=None, below=None, below_start=0):
    groups = [[p[j] for j in sorted(p)] for p in (pieces, below) if p is not None]
    starts = [start, below_start]
    count = groups[0][0].shape[0] - start if count is None else count
    lanes = groups[0][0].shape[1]
    block = max((b for b in range(16, 513, 16) if all(v % b == 0 for v in (count, *starts))), default=0)
    if lanes % 128 or not block:
        rows = [jnp.concatenate([v[at : at + count] for v in g], axis=1) for g, at in zip(groups, starts)]
        return jnp.concatenate(rows, axis=0)
    half = count // block
    specs = []
    for n, group in enumerate(groups):
        first = starts[n] // block

        def index(i, n=n, first=first):
            return (first + jnp.clip(i - n * half, 0, half - 1), 0)

        specs += [pl.BlockSpec((block, lanes), index)] * len(group)
    flat_groups = [v for g in groups for v in g]
    width = lanes * len(groups[0])
    return pl.pallas_call(
        functools.partial(join_kernel, half, [len(g) for g in groups]),
        grid=(half * len(groups),),
        in_specs=specs,
        out_specs=pl.BlockSpec((block, width), lambda i: (i, 0)),
        out_shape=jax.ShapeDtypeStruct((count * len(groups), width), flat_groups[0].dtype),
        cost_estimate=TINY,
        name="join",
    )(*flat_groups)


def shrink(total, held, bits):
    for bit in reversed(bits):
        at = {j: k for k, j in enumerate(held)}
        send = lane_blocks(total, len(held), [at[j] for j in held if j & bit])
        keep = lane_blocks(total, len(held), [at[j] for j in held if not j & bit])
        held = [j for j in held if not j & bit]
        total = (keep.astype(F32) + swap(send, "fsdp", 2 * bit).astype(F32)).astype(BF)
    return total, held


def minus_expm1(y):
    series = 1.0 + y * (1.0 / 7.0)
    for n in (6.0, 5.0, 4.0, 3.0, 2.0):
        series = 1.0 + y * (1.0 / n) * series
    return jnp.where(y > -0.35, -y * series, 1.0 - jnp.exp(y))


def sigmoid(v):
    return 0.5 * jnp.tanh(0.5 * v) + 0.5


def rows_iota(width):
    return lax.broadcasted_iota(jnp.int32, (8, width), 0)


def forward_kernel(
    branch,
    halo,
    conv_w,
    vectors,
    rate_w,
    inlet_w,
    conv_out,
    decay_out,
    local_out,
    prod_out,
    ext,
    rate_s,
    inlet_s,
):
    length, width = branch.shape[1:]
    ext[0:8] = halo[0]
    ext[8:] = branch[0]
    taps = conv_w.shape[0]

    def conv_step(i, carry):
        at = pl.multiple_of(i * STEP, STEP)
        window = ext[pl.ds(at, STEP + 8), :]
        total = jnp.broadcast_to(vectors[0:1, :], (STEP, width))
        for k in range(taps):
            total = total + conv_w[k : k + 1, :] * window[8 - k : 8 - k + STEP]
        conv_out[0, pl.ds(at, STEP), :] = total.astype(BF)
        return carry

    lax.fori_loop(0, length // STEP, conv_step, 0)
    mixed = conv_out[0]
    rate_s[...] = jnp.dot(mixed, rate_w[0], preferred_element_type=F32) + vectors[1:2, :]
    inlet_s[...] = jnp.dot(mixed, inlet_w[0], preferred_element_type=F32) + vectors[2:3, :]
    row = rows_iota(width)

    def scan_step(i, carry):
        at = pl.multiple_of(i * STEP, STEP)
        rows = pl.ds(at, STEP)
        rate = sigmoid(rate_s[rows, :])
        log_decay = (-DECAY_SCALE * rate) * vectors[3:4, :]
        decay = jnp.exp(log_decay)
        scale = jnp.sqrt(minus_expm1(2.0 * log_decay))
        source = scale * sigmoid(inlet_s[rows, :]) * conv_out[0, rows, :].astype(F32)
        decay_out[0, rows, :] = decay
        held, prod = carry
        for part in range(STEP // 8):
            a = decay[8 * part : 8 * part + 8]
            b = source[8 * part : 8 * part + 8]
            for k in (1, 2, 4):
                ok = row >= k
                b = jnp.where(ok, a * pltpu.roll(b, k, 0) + b, b)
                a = jnp.where(ok, a * pltpu.roll(a, k, 0), a)
            b = b + a * held
            a = a * prod
            here = pl.ds(at + 8 * part, 8)
            local_out[0, here, :] = b
            prod_out[0, here, :] = a
            held, prod = b[7:8], a[7:8]
        return held, prod

    lax.fori_loop(
        0,
        length // STEP,
        scan_step,
        (jnp.zeros((1, width), F32), jnp.ones((1, width), F32)),
    )


def block_spec(shape, index):
    return pl.BlockSpec(shape, index)


def run_forward(branch, halo, conv_w, vectors, rate_w, inlet_w):
    seqs, length, channels = branch.shape
    width = rate_w.shape[1]
    wide = pl.BlockSpec((1, length, width), lambda j, s: (s, 0, j))
    gate = pl.BlockSpec((1, width, width), lambda j, s: (j, 0, 0))
    full = lambda dt: jax.ShapeDtypeStruct(branch.shape, dt)
    return pl.pallas_call(
        forward_kernel,
        grid=(channels // width, seqs),
        in_specs=[
            wide,
            pl.BlockSpec((1, 8, width), lambda j, s: (s, 0, j)),
            pl.BlockSpec((conv_w.shape[0], width), lambda j, s: (0, j)),
            pl.BlockSpec((vectors.shape[0], width), lambda j, s: (0, j)),
            gate,
            gate,
        ],
        out_specs=[wide] * 4,
        out_shape=[full(BF), full(F32), full(F32), full(F32)],
        scratch_shapes=[
            pltpu.VMEM((length + 8, width), F32),
            pltpu.VMEM((length, width), F32),
            pltpu.VMEM((length, width), F32),
        ],
        cost_estimate=TINY,
        name="forward_scan",
    )(branch, halo, conv_w, vectors, rate_w, inlet_w)


def gelu_parts(x):
    square = x * x
    t = jnp.tanh(GELU_A * x * (1.0 + GELU_B * square))
    half = 0.5 * (1.0 + t)
    slope = half + 0.5 * x * (1.0 - t * t) * (GELU_A * (1.0 + 3.0 * GELU_B * square))
    return x * half, slope


def backward_scan_kernel(d_mixed, gate_pre, state, decay, d_gate, local_out, prod_out):
    length, width = state.shape[1:]
    row = rows_iota(width)

    def step(n, carry):
        at = pl.multiple_of(length - STEP - n * STEP, STEP)
        rows = pl.ds(at, STEP)
        dm = d_mixed[0, rows, :].astype(F32)
        act, slope = gelu_parts(gate_pre[0, rows, :])
        d_gate[0, rows, :] = (dm * state[0, rows, :] * slope).astype(BF)
        d_state = dm * act
        all_decay = decay[0, rows, :]
        held, prod, above = carry
        for part in reversed(range(STEP // 8)):
            plain = all_decay[8 * part : 8 * part + 8]
            a = jnp.where(row == 7, above, pltpu.roll(plain, 7, 0))
            b = d_state[8 * part : 8 * part + 8]
            for k in (1, 2, 4):
                ok = row < 8 - k
                b = jnp.where(ok, a * pltpu.roll(b, 8 - k, 0) + b, b)
                a = jnp.where(ok, a * pltpu.roll(a, 8 - k, 0), a)
            b = b + a * held
            a = a * prod
            here = pl.ds(at + 8 * part, 8)
            local_out[0, here, :] = b
            prod_out[0, here, :] = a
            held, prod, above = b[0:1], a[0:1], plain[0:1]
        return held, prod, above

    one = jnp.ones((1, width), F32)
    lax.fori_loop(0, length // STEP, step, (jnp.zeros((1, width), F32), one, one))


def run_backward_scan(d_mixed, gate_pre, state, decay, width):
    seqs, length, channels = state.shape
    wide = pl.BlockSpec((1, length, width), lambda j, s: (s, 0, j))
    full = lambda dt: jax.ShapeDtypeStruct(state.shape, dt)
    return pl.pallas_call(
        backward_scan_kernel,
        grid=(channels // width, seqs),
        in_specs=[wide] * 4,
        out_specs=[wide] * 3,
        out_shape=[full(BF), full(F32), full(F32)],
        cost_estimate=TINY,
        name="backward_scan",
    )(d_mixed, gate_pre, state, decay)


def backward_gates_kernel(
    local_c,
    prod_c,
    carry_in,
    state,
    state_in,
    conv_out,
    branch,
    halo,
    conv_w,
    vectors,
    rate_w,
    inlet_w,
    d_branch,
    head_out,
    tail_out,
    g_rate,
    g_inlet,
    sums,
    branch_x,
    state_x,
    rate_s,
    inlet_s,
    d_rate_s,
    d_inlet_s,
    d_conv_x,
):
    length, width = state.shape[1:]
    taps = conv_w.shape[0]
    seq = pl.program_id(1)
    branch_x[0:8] = halo[0]
    branch_x[8:] = branch[0]
    state_x[0:8] = jnp.broadcast_to(state_in[0], (8, width))
    state_x[8:] = state[0]
    mixed = conv_out[0]
    rate_s[...] = jnp.dot(mixed, rate_w[0], preferred_element_type=F32) + vectors[1:2, :]
    inlet_s[...] = jnp.dot(mixed, inlet_w[0], preferred_element_type=F32) + vectors[2:3, :]
    zero = jnp.zeros((8, width), F32)

    @pl.when(seq == 0)
    def _():
        g_rate[...] = jnp.zeros_like(g_rate)
        g_inlet[...] = jnp.zeros_like(g_inlet)
        sums[...] = jnp.zeros_like(sums)

    def fold(v):
        total = v[0:8]
        for part in range(1, STEP // 8):
            total = total + v[8 * part : 8 * part + 8]
        return total

    def gate_step(i, carry):
        s_decay, s_rate, s_inlet = carry
        at = pl.multiple_of(i * STEP, STEP)
        rows = pl.ds(at, STEP)
        rate = sigmoid(rate_s[rows, :])
        inlet = sigmoid(inlet_s[rows, :])
        log_decay = (-DECAY_SCALE * rate) * vectors[3:4, :]
        decay = jnp.exp(log_decay)
        scale = jnp.sqrt(minus_expm1(2.0 * log_decay))
        conv = conv_out[0, rows, :].astype(F32)
        cot = local_c[0, rows, :] + prod_c[0, rows, :] * carry_in[0]
        before = state_x[pl.ds(at, STEP + 8), :][7 : 7 + STEP]
        gated = cot * inlet
        d_log = cot * before * decay - gated * conv * (decay * decay) / scale
        weighted = d_log * rate
        d_rate = (weighted * (1.0 - rate) * (-DECAY_SCALE * vectors[3:4, :])).astype(BF)
        d_inlet = (gated * scale * conv * (1.0 - inlet)).astype(BF)
        d_rate_s[rows, :] = d_rate
        d_inlet_s[rows, :] = d_inlet
        d_conv_x[rows, :] = gated * scale
        return (
            s_decay + fold(weighted),
            s_rate + fold(d_rate.astype(F32)),
            s_inlet + fold(d_inlet.astype(F32)),
        )

    s_decay, s_rate, s_inlet = lax.fori_loop(0, length // STEP, gate_step, (zero, zero, zero))
    d_rate, d_inlet = d_rate_s[...], d_inlet_s[...]
    over_rows = (((0,), (0,)), ((), ()))
    transposed = (((1,), (1,)), ((), ()))
    g_rate[0] += lax.dot_general(mixed, d_rate, over_rows, preferred_element_type=F32)
    g_inlet[0] += lax.dot_general(mixed, d_inlet, over_rows, preferred_element_type=F32)
    d_conv_x[0:length] += lax.dot_general(
        d_rate, rate_w[0], transposed, preferred_element_type=F32
    ) + lax.dot_general(d_inlet, inlet_w[0], transposed, preferred_element_type=F32)
    d_conv_x[length:] = zero
    head_out[0] = d_conv_x[0:8]

    def conv_step(i, carry):
        at = pl.multiple_of(i * STEP, STEP)
        ahead = d_conv_x[pl.ds(at, STEP + 8), :]
        behind = branch_x[pl.ds(at, STEP + 8), :]
        here = ahead[0:STEP]
        total = conv_w[0:1, :] * here
        new = [carry[0] + fold(here)]
        for k in range(taps):
            if k:
                total = total + conv_w[k : k + 1, :] * ahead[k : k + STEP]
            new.append(carry[k + 1] + fold(here * behind[8 - k : 8 - k + STEP]))
        d_branch[0, pl.ds(at, STEP), :] = total.astype(BF)
        tail_out[0] = total[STEP - 8 : STEP]
        return tuple(new)

    found = lax.fori_loop(0, length // STEP, conv_step, (zero,) * (taps + 1))
    for k, total in enumerate((s_decay, s_rate, s_inlet, *found)):
        sums[k] += total


def run_backward_gates(
    local_c, prod_c, carry_in, state, state_in, conv_out, branch, halo, conv_w, vectors, rate_w, inlet_w
):
    seqs, length, channels = branch.shape
    width = rate_w.shape[1]
    taps = conv_w.shape[0]
    wide = pl.BlockSpec((1, length, width), lambda j, s: (s, 0, j))
    line = pl.BlockSpec((1, 1, width), lambda j, s: (s, 0, j))
    edge = pl.BlockSpec((1, 8, width), lambda j, s: (s, 0, j))
    gate = pl.BlockSpec((1, width, width), lambda j, s: (j, 0, 0))
    edge_shape = jax.ShapeDtypeStruct((seqs, 8, channels), F32)
    gate_shape = jax.ShapeDtypeStruct(rate_w.shape, F32)
    return pl.pallas_call(
        backward_gates_kernel,
        grid=(channels // width, seqs),
        in_specs=[
            wide,
            wide,
            line,
            wide,
            line,
            wide,
            wide,
            edge,
            pl.BlockSpec((taps, width), lambda j, s: (0, j)),
            pl.BlockSpec((vectors.shape[0], width), lambda j, s: (0, j)),
            gate,
            gate,
        ],
        out_specs=[
            wide,
            edge,
            edge,
            gate,
            gate,
            pl.BlockSpec((taps + 4, 8, width), lambda j, s: (0, 0, j)),
        ],
        out_shape=[
            jax.ShapeDtypeStruct(branch.shape, BF),
            edge_shape,
            edge_shape,
            gate_shape,
            gate_shape,
            jax.ShapeDtypeStruct((taps + 4, 8, channels), F32),
        ],
        scratch_shapes=[
            pltpu.VMEM((length + 8, width), F32),
            pltpu.VMEM((length + 8, width), F32),
            pltpu.VMEM((length, width), F32),
            pltpu.VMEM((length, width), F32),
            pltpu.VMEM((length, width), BF),
            pltpu.VMEM((length, width), BF),
            pltpu.VMEM((length + 8, width), F32),
        ],
        cost_estimate=TINY,
        name="backward_gates",
    )(local_c, prod_c, carry_in, state, state_in, conv_out, branch, halo, conv_w, vectors, rate_w, inlet_w)


def outer_kernel(values, cotangent, out):
    out[...] = lax.dot_general(
        values[...], cotangent[...], (((0,), (0,)), ((), ())), preferred_element_type=F32
    ).astype(BF)


def run_outer(values, cotangent):
    values = values.reshape(-1, values.shape[-1])
    cotangent = cotangent.reshape(-1, cotangent.shape[-1])
    rows, channels = values.shape
    width = cotangent.shape[1]
    block = 256 if channels % 256 == 0 else channels
    return pl.pallas_call(
        outer_kernel,
        grid=(channels // block,),
        in_specs=[
            pl.BlockSpec((rows, block), lambda i: (0, i)),
            pl.BlockSpec((rows, width), lambda i: (0, 0)),
        ],
        out_specs=pl.BlockSpec((block, width), lambda i: (i, 0)),
        out_shape=jax.ShapeDtypeStruct((channels, width), BF),
        cost_estimate=TINY,
        name="outer",
    )(values, cotangent)


def two_products_kernel(first, first_w, second, second_w, out):
    total = jnp.dot(first[...], first_w[...], preferred_element_type=F32)
    total = total + jnp.dot(second[...], second_w[...], preferred_element_type=F32)
    out[...] = total.astype(BF)


def run_two_products(first, first_w, second, second_w):
    lead = first.shape[:-1]
    inner = first.shape[-1]
    first, second = first.reshape(-1, inner), second.reshape(-1, inner)
    rows, width = first.shape[0], first_w.shape[1]
    block = 256 if width % 256 == 0 else width
    whole = pl.BlockSpec((rows, inner), lambda i: (0, 0))
    column = pl.BlockSpec((inner, block), lambda i: (0, i))
    total = pl.pallas_call(
        two_products_kernel,
        grid=(width // block,),
        in_specs=[whole, column, whole, column],
        out_specs=pl.BlockSpec((rows, block), lambda i: (0, i)),
        out_shape=jax.ShapeDtypeStruct((rows, width), BF),
        cost_estimate=TINY,
        name="two_products",
    )(first, first_w, second, second_w)
    return total.reshape(*lead, width)


def norm_back_kernel(values, gain, mine, other, direct, total, rounded, sums):
    v = values[...]
    inv_rms = lax.rsqrt(jnp.mean(v * v, axis=-1, keepdims=True) + EPS)
    unit = v * inv_rms
    cot = mine[...].astype(F32) + other[...].astype(F32)
    scaled = cot * gain[...]
    grad = inv_rms * (scaled - unit * jnp.mean(scaled * unit, axis=-1, keepdims=True))
    found = direct[...] + grad
    total[...] = found
    rounded[...] = found.astype(BF)

    @pl.when(pl.program_id(0) == 0)
    def _():
        sums[...] = jnp.zeros_like(sums)

    part = cot * unit
    fold = part[0:8]
    for row in range(8, part.shape[0], 8):
        fold = fold + part[row : row + 8]
    sums[...] += fold


def run_norm_back(values, gain_vec, mine, other, direct):
    shape = values.shape
    width = shape[-1]
    values, mine, other, direct = (v.reshape(-1, width) for v in (values, mine, other, direct))
    rows = values.shape[0]
    block = 128
    some = pl.BlockSpec((block, width), lambda i: (i, 0))
    total, rounded, sums = pl.pallas_call(
        norm_back_kernel,
        grid=(rows // block,),
        in_specs=[some, pl.BlockSpec((1, width), lambda i: (0, 0)), some, some, some],
        out_specs=[some, some, pl.BlockSpec((8, width), lambda i: (0, 0))],
        out_shape=[
            jax.ShapeDtypeStruct(values.shape, F32),
            jax.ShapeDtypeStruct(values.shape, BF),
            jax.ShapeDtypeStruct((8, width), F32),
        ],
        cost_estimate=TINY,
        name="norm_back",
    )(values, gain_vec[None], mine, other, direct)
    return total.reshape(shape), rounded.reshape(shape), jnp.sum(sums, axis=0)


def rms_norm(values, gain_vec):
    inv_rms = lax.rsqrt(jnp.mean(values * values, axis=-1, keepdims=True) + EPS)
    return values * inv_rms * gain_vec


def norm_back(values, gain_vec, cot):
    inv_rms = lax.rsqrt(jnp.mean(values * values, axis=-1, keepdims=True) + EPS)
    unit = values * inv_rms
    scaled = cot * gain_vec
    grad = inv_rms * (scaled - unit * jnp.mean(scaled * unit, axis=-1, keepdims=True))
    return grad, jnp.sum(cot * unit, axis=(0, 1))


def times(values, matrix, dtype=F32):
    return jnp.einsum("slk,kn->sln", values, matrix, preferred_element_type=dtype)


def times_t(values, matrix, dtype=F32):
    return jnp.einsum("sln,kn->slk", values, matrix, preferred_element_type=dtype)


def outer_sum(values, cotangent):
    return jnp.einsum("slk,sln->kn", values, cotangent, preferred_element_type=F32).astype(BF)


def shards(
    inputs,
    teacher,
    seq_lengths,
    first_gain,
    branch_weight,
    branch_bias,
    gate_weight,
    gate_bias,
    conv_weight,
    conv_bias,
    rate_weight,
    rate_bias,
    inlet_weight,
    inlet_bias,
    decay_param,
    out_weight,
    second_gain,
    geglu_gate,
    geglu_up,
    geglu_down,
):
    seq_dev, local_len, model_width = inputs.shape
    tp = lax.axis_size("tp")
    fsdp = lax.axis_size("fsdp")
    chips = fsdp // 2
    full_len = local_len * tp
    me = lax.axis_index("fsdp")
    z = lax.axis_index("tp")
    core = me & 1
    chip = me // 2
    width = rate_weight.shape[2]
    taps = conv_weight.shape[0]

    bits = bits_of(chips)
    near, far = bits[: len(bits) // 2], bits[len(bits) // 2 :]
    every = list(range(chips))

    def block_order(some):
        held = [0]
        for bit in some:
            held = sorted(held + [j ^ bit for j in held])
        return held

    lanes = 2 * model_width // fsdp
    half_r = branch_weight.shape[1] // 2
    half_f = geglu_gate.shape[1] // 2

    def same_chip(values):
        return swap(values, "fsdp", 1)

    def both_rows(values):
        return in_core_order(values, same_chip(values), core, 0)

    def units(matrices):
        def half(which):
            parts = [pick_half(m, which, axis) for m, axis in matrices]
            return jnp.concatenate([p.T if a == 1 else p for p, (_, a) in zip(parts, matrices)], axis=0)

        return in_core_order(half(core), same_chip(half(1 - core)), core, 1)

    x4 = both_rows(inputs)
    lengths4 = both_rows(seq_lengths)
    count = jnp.broadcast_to(jnp.sum(lengths4.astype(F32)), (8, 128))
    for b in bits:
        count = count + swap(count, "fsdp", 2 * b)
    valid_total = count[0, 0]
    unit_r = units([(branch_weight, 1), (gate_weight, 1), (out_weight, 0)])
    unit_f = units([(geglu_gate, 1), (geglu_up, 1), (geglu_down, 0)])

    rows_chip = 2 * rate_weight.shape[1]
    pair_size = 2 * rows_chip * width
    pair_lines = -(-pair_size // (16 * lanes)) * 16
    pair = jnp.concatenate([rate_weight, inlet_weight], axis=1)
    unit_p = in_core_order(
        pick_half(pair, core, 0).reshape(2, -1, width),
        same_chip(pick_half(pair, 1 - core, 0)).reshape(2, -1, width),
        core,
        1,
    )
    unit_p = jnp.pad(unit_p.reshape(-1), (0, pair_lines * lanes - pair_size)).reshape(pair_lines, lanes)

    def all_z(values):
        return lax.all_gather(values, "tp", axis=0, tiled=False)

    def flat(values):
        return values.reshape(-1, values.shape[-1])

    top = tp // 2

    def rows_of(gathered, start, count, blocks=slice(None)):
        return flat(gathered[blocks, start : start + count])

    first_z = all_z(jnp.concatenate([unit_r[: 2 * half_r], unit_p], axis=0))
    second_z = all_z(after(unit_f[: 2 * half_f], first_z))
    out_own = unit_r[2 * half_r :]
    out_parts = {0: out_own} | {j: swap(out_own, "fsdp", 2 * j) for j in every[1:]}
    first_z, x4, lengths4, valid_total, out_parts = fence(first_z, x4, lengths4, valid_total, out_parts)
    a1 = jnp.concatenate([rows_of(first_z, 0, half_r), rows_of(first_z, 2 * half_r, pair_lines)], axis=0)
    b1 = rows_of(first_z, half_r, half_r)
    left_a, left_b = block_order(near), block_order(far)
    a1, b1 = spread({0: a1}, near), spread({0: b1}, far)
    first_a, first_b = a1[near[-1]], b1[far[-1]]
    a1, b1 = spread(a1, far), spread(b1, near)
    a3, b3 = {0: rows_of(second_z, 0, half_f)}, {0: rows_of(second_z, half_f, half_f)}
    local_vectors = jnp.concatenate(
        [
            conv_weight,
            jnp.stack([branch_bias, gate_bias, conv_bias, rate_bias, inlet_bias, decay_param]),
        ],
        axis=0,
    )
    held = pick_half(after(local_vectors, first_a, first_b), core, 1)
    for b in bits_of(tp):
        held = jnp.concatenate([held, swap(held, "tp", b)], axis=1)
    held = xor_blocks(held, 1, tp, z)

    def to_chip(values):
        return xor_blocks(values, values.ndim - 1, chips, chip)

    gain1, gain2 = to_chip(first_gain), to_chip(second_gain)
    x4 = to_chip(x4)
    residual = x4.astype(F32)
    first_rows = rms_norm(residual, gain1).astype(BF)
    a1, b1, a3, b3, held, first_rows = fence(a1, b1, a3, b3, held, first_rows)
    out_z = all_z(after(join(out_parts), second_z, a1[0]))
    third_z = all_z(after(unit_f[2 * half_f :], out_z))
    a3, b3 = spread(a3, near), spread(b3, far)
    far_a = {k ^ j: swap(a3[k], "fsdp", 2 * j) for k in [0] for j in far[:1]}
    near_b = {k ^ j: swap(b3[k], "fsdp", 2 * j) for k in [0] for j in near[:1]}
    size_r = tp * half_r
    w_branch, w_gate = join(a1, 0, size_r), join(b1, 0, size_r)
    w_out = flat(out_z)
    w_pair = [a1[j][size_r : size_r + tp * pair_lines].reshape(tp, -1)[:, :pair_size] for j in every]
    w_pair = jnp.stack(w_pair, axis=1).reshape(tp, chips, 2, rows_chip, width)
    w_pair = xor_blocks(w_pair, 1, chips, chip).transpose(2, 0, 1, 3, 4).reshape(2, tp, chips * rows_chip, width)
    w_rate, w_inlet = w_pair[0], w_pair[1]

    taps_w = held[:taps]
    b_branch, b_gate, b_conv, b_rate, b_inlet, decay_vec = (held[taps + k] for k in range(6))
    soft = jax.nn.softplus(-decay_vec)
    vectors = jnp.stack([b_conv, b_rate, b_inlet, soft])

    branch_pre = times_t(first_rows, w_branch) + b_branch

    def along_z(values, shift):
        return lax.ppermute(values, "tp", [(i, i + shift) for i in range(tp) if 0 <= i + shift < tp])

    halo = jnp.pad(along_z(branch_pre[:, local_len - taps + 1 :], 1), ((0, 0), (8 - taps + 1, 0), (0, 0)))
    conv_out, decay_rate, local_state, prod_decay = run_forward(
        branch_pre, halo, taps_w, vectors, w_rate, w_inlet
    )
    ends = jnp.stack([prod_decay[:, -1], local_state[:, -1]])
    state_in = jnp.zeros_like(ends[0])
    for shift in reversed(range(1, tp)):
        got = along_z(ends, shift)
        state_in = got[1] + got[0] * state_in
    state_in = state_in[:, None]
    state_in, a3, b3, far_a, near_b = fence(state_in, a3, b3, far_a, near_b)
    gate_pre = times_t(after(first_rows, state_in), w_gate) + b_gate
    a3, b3 = finish(a3, far_a, far), finish(b3, near_b, near)
    state = local_state + prod_decay * state_in
    mixed = (state * jax.nn.gelu(gate_pre)).astype(BF)
    def core_sum(term):
        return term.astype(F32) + same_chip(term).astype(F32)

    out_term, a3, b3, third_z = fence(times(mixed, w_out, BF), a3, b3, third_z)
    a4, b4 = {0: flat(third_z[:top])}, {0: flat(third_z[top:])}
    a4, b4 = spread(a4, near), spread(b4, far)
    w_ffgate, w_ffup = join(a3), join(b3)
    middle = residual + core_sum(out_term)
    second_rows = rms_norm(middle, gain2).astype(BF)
    second_rows, a4, b4 = fence(second_rows, a4, b4)
    a4, b4 = spread(a4, far), spread(b4, near)
    teacher4 = both_rows(after(teacher, second_rows))
    ff_gate = times_t(second_rows, w_ffgate)
    ff_up = times_t(second_rows, w_ffup)
    ff_hidden = (jax.nn.gelu(ff_gate) * ff_up).astype(BF)
    ff_hidden, a4, b4, teacher4 = fence(ff_hidden, a4, b4, teacher4)
    w_ffdown = join(a4, 0, None, b4, 0)
    final = middle + core_sum(times(ff_hidden, w_ffdown, BF))

    positions = z * local_len + jnp.arange(local_len, dtype=jnp.int32)
    valid_mask = (positions[None, :] < lengths4[:, None]).astype(F32)[..., None]
    teacher4 = to_chip(teacher4).astype(F32)
    mismatch = final - teacher4
    loss_part = jnp.sum(valid_mask * mismatch * mismatch)
    scaling = seq_dev * fsdp * full_len / valid_total
    out_cot = valid_mask * mismatch * scaling
    ff_cot = out_cot.astype(BF)

    def by_z(a, b):
        return lax.psum_scatter(
            jnp.concatenate([a.reshape(tp, -1, lanes), b.reshape(tp, -1, lanes)], axis=1),
            "tp",
            scatter_dimension=0,
            tiled=False,
        )

    def halves(grad):
        return jnp.split(grad, 2, axis=0)

    def far_first(grad):
        return shrink(grad, every, far)[0]

    def near_first(grad):
        return shrink(grad, every, near)[0]

    def far_last(grad):
        return shrink(grad, left_b, far)[0]

    def near_last(grad):
        return shrink(grad, left_a, near)[0]

    ff_cot, g_ffdown = fence(ff_cot, outer_sum(ff_hidden, ff_cot))
    down_sum = lax.psum_scatter(g_ffdown.reshape(tp, half_f, model_width), "tp", scatter_dimension=0, tiled=False)
    d_hidden = times_t(ff_cot, w_ffdown)
    act, slope = gelu_parts(ff_gate)
    d_up = (d_hidden * act).astype(BF)
    d_ffgate = (d_hidden * ff_up * slope).astype(BF)
    g_ffgate = run_outer(d_ffgate, second_rows)
    d_ffgate, d_up, g_ffgate = fence(d_ffgate, d_up, g_ffgate)
    top_g, low_g = halves(g_ffgate)
    a3, b3 = far_first(top_g), near_first(low_g)
    g_ffup = run_outer(d_up, second_rows)
    d_second = run_two_products(d_ffgate, w_ffgate, after(d_up, g_ffup), w_ffup)
    d_second, a3, b3, g_ffup = fence(d_second, a3, b3, g_ffup)
    top_u, low_u = halves(g_ffup)
    a6, b6 = far_first(top_u), near_first(low_u)
    d_middle, mid_cot, g_second = run_norm_back(middle, gain2, d_second, same_chip(d_second), out_cot)
    mid_cot, a3, b3, a6, b6 = fence(mid_cot, a3, b3, a6, b6)
    a3, b3 = near_last(jnp.concatenate([a3, a6], axis=0)), far_last(jnp.concatenate([b3, b6], axis=0))
    d_mixed = times_t(mid_cot, w_out)
    d_gate, local_c, prod_c = run_backward_scan(d_mixed, gate_pre, state, decay_rate, width)
    d_gate, local_c, prod_c, a3, b3, down_sum = fence(d_gate, local_c, prod_c, a3, b3, down_sum)
    unit_gu = jnp.concatenate([a3.reshape(2, -1, half_f, lanes), b3.reshape(2, -1, half_f, lanes)], axis=1)
    unit_gu = unit_gu.transpose(1, 0, 2, 3).reshape(tp, -1, lanes)
    unit_gu = lax.psum_scatter(unit_gu, "tp", scatter_dimension=0, tiled=False)
    top_d, low_d = halves(down_sum)
    a4, b4 = far_first(top_d), near_first(low_d)
    starts = jnp.stack([prod_c[:, 0], local_c[:, 0]]) * decay_rate[:, 0]
    carry_in = jnp.zeros_like(starts[0])
    for shift in reversed(range(1, tp)):
        got = along_z(starts, -shift)
        carry_in = got[1] + got[0] * carry_in
    g_out = outer_sum(after(mixed, d_gate), mid_cot)
    g_gate = outer_sum(d_gate, first_rows)
    local_c, g_gate, g_out, a4, b4 = fence(local_c, g_gate, g_out, a4, b4)
    a4, b4 = near_last(a4), far_last(b4)
    a2, b1 = far_first(g_out), near_first(g_gate)
    d_branch, head, tail, g_rate, g_inlet, sums = run_backward_gates(
        local_c,
        prod_c,
        carry_in[:, None],
        state,
        state_in,
        conv_out,
        branch_pre,
        halo,
        taps_w,
        vectors,
        w_rate,
        w_inlet,
    )
    d_branch, head, a2, b1, a4, b4, unit_gu = fence(d_branch, head, a2, b1, a4, b4, unit_gu)
    unit_d = jnp.concatenate([a4, b4], axis=0)
    ahead = along_z(head[:, : taps - 1], -1)
    edge = tail[:, 8 - taps + 1 :]
    for k in range(1, taps):
        first = taps - 1 - k
        edge = edge.at[:, first:].add(taps_w[k] * ahead[:, :k])
    d_branch = lax.dynamic_update_slice(d_branch, edge.astype(BF), (0, local_len - taps + 1, 0))

    a2, b1 = near_last(a2), far_last(b1)
    g_branch = outer_sum(d_branch, first_rows)
    g_rate, g_inlet, d_branch, a2, b1, g_branch = fence(g_rate, g_inlet, d_branch, a2, b1, g_branch)
    unit_og = by_z(a2, b1)
    top_b, low_b = halves(g_branch)
    a1, b5 = far_first(top_b), near_first(low_b)
    g_pair = jnp.stack([g_rate, g_inlet]).reshape(2, tp, chips, rows_chip, width)
    g_pair = xor_blocks(g_pair, 2, chips, chip).astype(BF).transpose(1, 2, 0, 3, 4).reshape(tp, chips, -1)
    g_pair = jnp.pad(g_pair, ((0, 0), (0, 0), (0, pair_lines * lanes - pair_size)))
    g_pair = g_pair.reshape(tp, chips, pair_lines, lanes).transpose(0, 2, 1, 3).reshape(-1, model_width)
    g_pair, a1, b5 = fence(g_pair, a1, b5)
    top_p, low_p = halves(g_pair)
    ap, bp = far_first(top_p), near_first(low_p)
    a1, b5 = near_last(a1), far_last(b5)
    d_first_part = (times(d_branch, w_branch) + times(d_gate, w_gate)).astype(BF)
    d_first_part, a1, b5, ap, bp, unit_og = fence(d_first_part, a1, b5, ap, bp, unit_og)
    ap, bp = near_last(ap), far_last(bp)
    unit_b = [jnp.concatenate(v, axis=0).reshape(tp, -1, lanes) for v in ((a1, b5), (ap, bp))]
    unit_b = lax.psum_scatter(jnp.concatenate(unit_b, axis=1), "tp", scatter_dimension=0, tiled=False)

    def own(values):
        return pick_half(values, core, 0)

    d_first = own(d_first_part).astype(F32) + same_chip(pick_half(d_first_part, 1 - core, 0)).astype(F32)
    d_in_norm, g_first = norm_back(own(residual), gain1, d_first)
    input_grad = to_chip(own(d_middle) + d_in_norm)
    block_out = to_chip(own(final).astype(BF))

    def to_own(grad, channel_axis):
        mine = pick_half(grad, core, 1)
        other = same_chip(pick_half(grad, 1 - core, 1))
        whole = in_core_order(mine, other, core, 0)
        return (whole.T if channel_axis == 1 else whole).astype(F32)

    pair_g = unit_b[half_r:].reshape(-1)[:pair_size].reshape(2, rows_chip, width)
    pair_g = in_core_order(
        pick_half(pair_g, core, 1)[None], same_chip(pick_half(pair_g, 1 - core, 1))[None], core, 0
    ).astype(F32)

    sums = jnp.sum(sums, axis=1)
    small = jnp.concatenate(
        [
            jnp.stack(
                [
                    jnp.sum(d_branch.astype(F32), axis=(0, 1)),
                    jnp.sum(d_gate.astype(F32), axis=(0, 1)),
                    sums[0] * (DECAY_SCALE * jax.nn.sigmoid(-decay_vec)),
                ]
            ),
            sums[1:],
        ],
        axis=0,
    )
    found = jnp.concatenate(
        [
            to_chip(g_first),
            to_chip(0.5 * g_second),
            jnp.broadcast_to(0.5 * loss_part, (128,)),
            small.reshape(-1),
        ]
    ).reshape(-1, 128)
    for b in bits:
        found = found + swap(found, "fsdp", 2 * b)
    for b in bits_of(tp):
        found = found + swap(found, "tp", b)
    other = same_chip(found)
    lines = (2 * model_width + 128) // 128
    stats = (found[:lines] + other[:lines]).reshape(-1)
    block = lambda v: lax.dynamic_index_in_dim(v[lines:].reshape(small.shape[0], tp, half_r), z, 1, keepdims=False)
    small = in_core_order(block(found), block(other), core, 1)
    loss_value = stats[2 * model_width] / (model_width * valid_total)
    return (
        block_out,
        loss_value,
        input_grad,
        stats[:model_width],
        to_own(unit_b[:half_r], 1),
        small[0],
        to_own(unit_og[half_r:], 1),
        small[1],
        small[6:],
        small[5],
        pair_g[:, 0],
        small[3],
        pair_g[:, 1],
        small[4],
        small[2],
        to_own(unit_og[:half_r], 0),
        stats[model_width : 2 * model_width],
        to_own(unit_gu[:half_f], 1),
        to_own(unit_gu[half_f:], 1),
        to_own(unit_d, 0),
    )


def solution(mesh):
    rows = P("fsdp", "tp", None)
    by_column, by_row = P("fsdp", "tp"), P("tp", "fsdp")
    blocks = P("tp", "fsdp", None)
    channel = P("tp")
    return jax.shard_map(
        shards,
        mesh=mesh,
        in_specs=(
            rows,
            rows,
            P("fsdp"),
            P(),
            by_column,
            channel,
            by_column,
            channel,
            P(None, "tp"),
            channel,
            blocks,
            channel,
            blocks,
            channel,
            channel,
            by_row,
            P(),
            by_column,
            by_column,
            by_row,
        ),
        out_specs=(
            rows,
            P(),
            rows,
            P(),
            by_column,
            channel,
            by_column,
            channel,
            P(None, "tp"),
            channel,
            blocks,
            channel,
            blocks,
            channel,
            channel,
            by_row,
            P(),
            by_column,
            by_column,
            by_row,
        ),
        check_vma=False,
    )
```

```python
import functools

import jax
import jax.numpy as jnp
from jax import lax
from jax.experimental import pallas as pl
from jax.experimental.pallas import tpu as pltpu
from jax.sharding import PartitionSpec as P

EPS = 1e-06
DECAY_SCALE = 8.0
BF = jnp.bfloat16
F32 = jnp.float32
STEP = 16
GELU_A = 0.7978845608028654
GELU_B = 0.044715
TINY = pl.CostEstimate(flops=1, bytes_accessed=1, transcendentals=0)


def swap(values, axis_name, bit):
    size = lax.axis_size(axis_name)
    return lax.ppermute(values, axis_name, [(i, i ^ bit) for i in range(size)])


def bits_of(count):
    return [1 << b for b in range(count.bit_length() - 1)]


def in_core_order(mine, other, core, axis):
    first = jnp.where(core == 0, mine, other)
    second = jnp.where(core == 0, other, mine)
    return jnp.concatenate([first, second], axis=axis)


def pick_half(values, which, axis):
    low, high = jnp.split(values, 2, axis=axis)
    return jnp.where(which == 0, low, high)


def xor_blocks(values, axis, count, index):
    blocks = jnp.split(values, count, axis=axis)
    for bit in bits_of(count):
        flipped = (index & bit) != 0
        blocks = [jnp.where(flipped, blocks[j ^ bit], blocks[j]) for j in range(count)]
    return jnp.concatenate(blocks, axis=axis)


def lane_blocks(values, count, wanted):
    width = values.shape[1] // count
    runs, start = [], 0
    while start < len(wanted):
        stop = start + 1
        while stop < len(wanted) and wanted[stop] == wanted[stop - 1] + 1:
            stop += 1
        runs.append(values[:, wanted[start] * width : (wanted[stop - 1] + 1) * width])
        start = stop
    return runs[0] if len(runs) == 1 else jnp.concatenate(runs, axis=1)


def after(value, *others):
    return lax.optimization_barrier((value, *others))[0]


def spread(pieces, bits):
    for bit in bits:
        held = sorted(pieces)
        if len(held) <= 2:
            got = {j ^ bit: swap(pieces[j], "fsdp", 2 * bit) for j in held}
        else:
            other = swap(jnp.concatenate([pieces[j] for j in held], axis=1), "fsdp", 2 * bit)
            width = pieces[held[0]].shape[1]
            got = {j ^ bit: other[:, k * width : (k + 1) * width] for k, j in enumerate(held)}
        pieces = pieces | got
    return pieces


def finish(pieces, ahead, bits):
    for bit in bits:
        got = {j ^ bit: swap(v, "fsdp", 2 * bit) for j, v in pieces.items() if j ^ bit not in ahead}
        pieces = pieces | ahead | got
        ahead = {}
    return pieces


def fence(*groups):
    return lax.optimization_barrier(groups)


def join_kernel(half, counts, *refs):
    out = refs[-1]
    first, second = refs[: counts[0]], refs[counts[0] : -1]

    def put(parts):
        width = parts[0].shape[1]
        for k, part in enumerate(parts):
            out[:, k * width : (k + 1) * width] = part[...]

    if not second:
        put(first)
        return
    pl.when(pl.program_id(0) < half)(lambda: put(first))
    pl.when(pl.program_id(0) >= half)(lambda: put(second))


def join(pieces, start=0, count=None, below=None, below_start=0):
    groups = [[p[j] for j in sorted(p)] for p in (pieces, below) if p is not None]
    starts = [start, below_start]
    count = groups[0][0].shape[0] - start if count is None else count
    lanes = groups[0][0].shape[1]
    block = max((b for b in range(16, 513, 16) if all(v % b == 0 for v in (count, *starts))), default=0)
    if lanes % 128 or not block:
        rows = [jnp.concatenate([v[at : at + count] for v in g], axis=1) for g, at in zip(groups, starts)]
        return jnp.concatenate(rows, axis=0)
    half = count // block
    specs = []
    for n, group in enumerate(groups):
        first = starts[n] // block

        def index(i, n=n, first=first):
            return (first + jnp.clip(i - n * half, 0, half - 1), 0)

        specs += [pl.BlockSpec((block, lanes), index)] * len(group)
    flat_groups = [v for g in groups for v in g]
    width = lanes * len(groups[0])
    return pl.pallas_call(
        functools.partial(join_kernel, half, [len(g) for g in groups]),
        grid=(half * len(groups),),
        in_specs=specs,
        out_specs=pl.BlockSpec((block, width), lambda i: (i, 0)),
        out_shape=jax.ShapeDtypeStruct((count * len(groups), width), flat_groups[0].dtype),
        cost_estimate=TINY,
        name="join",
    )(*flat_groups)


def shrink(total, held, bits):
    for bit in reversed(bits):
        at = {j: k for k, j in enumerate(held)}
        send = lane_blocks(total, len(held), [at[j] for j in held if j & bit])
        keep = lane_blocks(total, len(held), [at[j] for j in held if not j & bit])
        held = [j for j in held if not j & bit]
        total = (keep.astype(F32) + swap(send, "fsdp", 2 * bit).astype(F32)).astype(BF)
    return total, held


def minus_expm1(y):
    series = 1.0 + y * (1.0 / 7.0)
    for n in (6.0, 5.0, 4.0, 3.0, 2.0):
        series = 1.0 + y * (1.0 / n) * series
    return jnp.where(y > -0.35, -y * series, 1.0 - jnp.exp(y))


def sigmoid(v):
    return 0.5 * jnp.tanh(0.5 * v) + 0.5


def rows_iota(width):
    return lax.broadcasted_iota(jnp.int32, (8, width), 0)


def forward_kernel(
    branch,
    halo,
    conv_w,
    vectors,
    rate_w,
    inlet_w,
    conv_out,
    decay_out,
    local_out,
    prod_out,
    ext,
    rate_s,
    inlet_s,
):
    length, width = branch.shape[1:]
    ext[0:8] = halo[0]
    ext[8:] = branch[0]
    taps = conv_w.shape[0]

    def conv_step(i, carry):
        at = pl.multiple_of(i * STEP, STEP)
        window = ext[pl.ds(at, STEP + 8), :]
        total = jnp.broadcast_to(vectors[0:1, :], (STEP, width))
        for k in range(taps):
            total = total + conv_w[k : k + 1, :] * window[8 - k : 8 - k + STEP]
        conv_out[0, pl.ds(at, STEP), :] = total.astype(BF)
        return carry

    lax.fori_loop(0, length // STEP, conv_step, 0)
    mixed = conv_out[0]
    rate_s[...] = jnp.dot(mixed, rate_w[0], preferred_element_type=F32) + vectors[1:2, :]
    inlet_s[...] = jnp.dot(mixed, inlet_w[0], preferred_element_type=F32) + vectors[2:3, :]
    row = rows_iota(width)

    def scan_step(i, carry):
        at = pl.multiple_of(i * STEP, STEP)
        rows = pl.ds(at, STEP)
        rate = sigmoid(rate_s[rows, :])
        log_decay = (-DECAY_SCALE * rate) * vectors[3:4, :]
        decay = jnp.exp(log_decay)
        scale = jnp.sqrt(minus_expm1(2.0 * log_decay))
        source = scale * sigmoid(inlet_s[rows, :]) * conv_out[0, rows, :].astype(F32)
        decay_out[0, rows, :] = decay
        held, prod = carry
        for part in range(STEP // 8):
            a = decay[8 * part : 8 * part + 8]
            b = source[8 * part : 8 * part + 8]
            for k in (1, 2, 4):
                ok = row >= k
                b = jnp.where(ok, a * pltpu.roll(b, k, 0) + b, b)
                a = jnp.where(ok, a * pltpu.roll(a, k, 0), a)
            b = b + a * held
            a = a * prod
            here = pl.ds(at + 8 * part, 8)
            local_out[0, here, :] = b
            prod_out[0, here, :] = a
            held, prod = b[7:8], a[7:8]
        return held, prod

    lax.fori_loop(
        0,
        length // STEP,
        scan_step,
        (jnp.zeros((1, width), F32), jnp.ones((1, width), F32)),
    )


def block_spec(shape, index):
    return pl.BlockSpec(shape, index)


def run_forward(branch, halo, conv_w, vectors, rate_w, inlet_w):
    seqs, length, channels = branch.shape
    width = rate_w.shape[1]
    wide = pl.BlockSpec((1, length, width), lambda j, s: (s, 0, j))
    gate = pl.BlockSpec((1, width, width), lambda j, s: (j, 0, 0))
    full = lambda dt: jax.ShapeDtypeStruct(branch.shape, dt)
    return pl.pallas_call(
        forward_kernel,
        grid=(channels // width, seqs),
        in_specs=[
            wide,
            pl.BlockSpec((1, 8, width), lambda j, s: (s, 0, j)),
            pl.BlockSpec((conv_w.shape[0], width), lambda j, s: (0, j)),
            pl.BlockSpec((vectors.shape[0], width), lambda j, s: (0, j)),
            gate,
            gate,
        ],
        out_specs=[wide] * 4,
        out_shape=[full(BF), full(F32), full(F32), full(F32)],
        scratch_shapes=[
            pltpu.VMEM((length + 8, width), F32),
            pltpu.VMEM((length, width), F32),
            pltpu.VMEM((length, width), F32),
        ],
        cost_estimate=TINY,
        name="forward_scan",
    )(branch, halo, conv_w, vectors, rate_w, inlet_w)


def gelu_parts(x):
    square = x * x
    t = jnp.tanh(GELU_A * x * (1.0 + GELU_B * square))
    half = 0.5 * (1.0 + t)
    slope = half + 0.5 * x * (1.0 - t * t) * (GELU_A * (1.0 + 3.0 * GELU_B * square))
    return x * half, slope


def backward_scan_kernel(d_mixed, gate_pre, state, decay, d_gate, local_out, prod_out):
    length, width = state.shape[1:]
    row = rows_iota(width)

    def step(n, carry):
        at = pl.multiple_of(length - STEP - n * STEP, STEP)
        rows = pl.ds(at, STEP)
        dm = d_mixed[0, rows, :].astype(F32)
        act, slope = gelu_parts(gate_pre[0, rows, :])
        d_gate[0, rows, :] = (dm * state[0, rows, :] * slope).astype(BF)
        d_state = dm * act
        all_decay = decay[0, rows, :]
        held, prod, above = carry
        for part in reversed(range(STEP // 8)):
            plain = all_decay[8 * part : 8 * part + 8]
            a = jnp.where(row == 7, above, pltpu.roll(plain, 7, 0))
            b = d_state[8 * part : 8 * part + 8]
            for k in (1, 2, 4):
                ok = row < 8 - k
                b = jnp.where(ok, a * pltpu.roll(b, 8 - k, 0) + b, b)
                a = jnp.where(ok, a * pltpu.roll(a, 8 - k, 0), a)
            b = b + a * held
            a = a * prod
            here = pl.ds(at + 8 * part, 8)
            local_out[0, here, :] = b
            prod_out[0, here, :] = a
            held, prod, above = b[0:1], a[0:1], plain[0:1]
        return held, prod, above

    one = jnp.ones((1, width), F32)
    lax.fori_loop(0, length // STEP, step, (jnp.zeros((1, width), F32), one, one))


def run_backward_scan(d_mixed, gate_pre, state, decay, width):
    seqs, length, channels = state.shape
    wide = pl.BlockSpec((1, length, width), lambda j, s: (s, 0, j))
    full = lambda dt: jax.ShapeDtypeStruct(state.shape, dt)
    return pl.pallas_call(
        backward_scan_kernel,
        grid=(channels // width, seqs),
        in_specs=[wide] * 4,
        out_specs=[wide] * 3,
        out_shape=[full(BF), full(F32), full(F32)],
        cost_estimate=TINY,
        name="backward_scan",
    )(d_mixed, gate_pre, state, decay)


def backward_gates_kernel(
    local_c,
    prod_c,
    carry_in,
    state,
    state_in,
    conv_out,
    branch,
    halo,
    conv_w,
    vectors,
    rate_w,
    inlet_w,
    d_branch,
    head_out,
    tail_out,
    g_rate,
    g_inlet,
    sums,
    branch_x,
    state_x,
    rate_s,
    inlet_s,
    d_rate_s,
    d_inlet_s,
    d_conv_x,
):
    length, width = state.shape[1:]
    taps = conv_w.shape[0]
    seq = pl.program_id(1)
    branch_x[0:8] = halo[0]
    branch_x[8:] = branch[0]
    state_x[0:8] = jnp.broadcast_to(state_in[0], (8, width))
    state_x[8:] = state[0]
    mixed = conv_out[0]
    rate_s[...] = jnp.dot(mixed, rate_w[0], preferred_element_type=F32) + vectors[1:2, :]
    inlet_s[...] = jnp.dot(mixed, inlet_w[0], preferred_element_type=F32) + vectors[2:3, :]
    zero = jnp.zeros((8, width), F32)

    @pl.when(seq == 0)
    def _():
        g_rate[...] = jnp.zeros_like(g_rate)
        g_inlet[...] = jnp.zeros_like(g_inlet)
        sums[...] = jnp.zeros_like(sums)

    def fold(v):
        total = v[0:8]
        for part in range(1, STEP // 8):
            total = total + v[8 * part : 8 * part + 8]
        return total

    def gate_step(i, carry):
        s_decay, s_rate, s_inlet = carry
        at = pl.multiple_of(i * STEP, STEP)
        rows = pl.ds(at, STEP)
        rate = sigmoid(rate_s[rows, :])
        inlet = sigmoid(inlet_s[rows, :])
        log_decay = (-DECAY_SCALE * rate) * vectors[3:4, :]
        decay = jnp.exp(log_decay)
        scale = jnp.sqrt(minus_expm1(2.0 * log_decay))
        conv = conv_out[0, rows, :].astype(F32)
        cot = local_c[0, rows, :] + prod_c[0, rows, :] * carry_in[0]
        before = state_x[pl.ds(at, STEP + 8), :][7 : 7 + STEP]
        gated = cot * inlet
        d_log = cot * before * decay - gated * conv * (decay * decay) / scale
        weighted = d_log * rate
        d_rate = (weighted * (1.0 - rate) * (-DECAY_SCALE * vectors[3:4, :])).astype(BF)
        d_inlet = (gated * scale * conv * (1.0 - inlet)).astype(BF)
        d_rate_s[rows, :] = d_rate
        d_inlet_s[rows, :] = d_inlet
        d_conv_x[rows, :] = gated * scale
        return (
            s_decay + fold(weighted),
            s_rate + fold(d_rate.astype(F32)),
            s_inlet + fold(d_inlet.astype(F32)),
        )

    s_decay, s_rate, s_inlet = lax.fori_loop(0, length // STEP, gate_step, (zero, zero, zero))
    d_rate, d_inlet = d_rate_s[...], d_inlet_s[...]
    over_rows = (((0,), (0,)), ((), ()))
    transposed = (((1,), (1,)), ((), ()))
    g_rate[0] += lax.dot_general(mixed, d_rate, over_rows, preferred_element_type=F32)
    g_inlet[0] += lax.dot_general(mixed, d_inlet, over_rows, preferred_element_type=F32)
    d_conv_x[0:length] += lax.dot_general(
        d_rate, rate_w[0], transposed, preferred_element_type=F32
    ) + lax.dot_general(d_inlet, inlet_w[0], transposed, preferred_element_type=F32)
    d_conv_x[length:] = zero
    head_out[0] = d_conv_x[0:8]

    def conv_step(i, carry):
        at = pl.multiple_of(i * STEP, STEP)
        ahead = d_conv_x[pl.ds(at, STEP + 8), :]
        behind = branch_x[pl.ds(at, STEP + 8), :]
        here = ahead[0:STEP]
        total = conv_w[0:1, :] * here
        new = [carry[0] + fold(here)]
        for k in range(taps):
            if k:
                total = total + conv_w[k : k + 1, :] * ahead[k : k + STEP]
            new.append(carry[k + 1] + fold(here * behind[8 - k : 8 - k + STEP]))
        d_branch[0, pl.ds(at, STEP), :] = total.astype(BF)
        tail_out[0] = total[STEP - 8 : STEP]
        return tuple(new)

    found = lax.fori_loop(0, length // STEP, conv_step, (zero,) * (taps + 1))
    for k, total in enumerate((s_decay, s_rate, s_inlet, *found)):
        sums[k] += total


def run_backward_gates(
    local_c, prod_c, carry_in, state, state_in, conv_out, branch, halo, conv_w, vectors, rate_w, inlet_w
):
    seqs, length, channels = branch.shape
    width = rate_w.shape[1]
    taps = conv_w.shape[0]
    wide = pl.BlockSpec((1, length, width), lambda j, s: (s, 0, j))
    line = pl.BlockSpec((1, 1, width), lambda j, s: (s, 0, j))
    edge = pl.BlockSpec((1, 8, width), lambda j, s: (s, 0, j))
    gate = pl.BlockSpec((1, width, width), lambda j, s: (j, 0, 0))
    edge_shape = jax.ShapeDtypeStruct((seqs, 8, channels), F32)
    gate_shape = jax.ShapeDtypeStruct(rate_w.shape, F32)
    return pl.pallas_call(
        backward_gates_kernel,
        grid=(channels // width, seqs),
        in_specs=[
            wide,
            wide,
            line,
            wide,
            line,
            wide,
            wide,
            edge,
            pl.BlockSpec((taps, width), lambda j, s: (0, j)),
            pl.BlockSpec((vectors.shape[0], width), lambda j, s: (0, j)),
            gate,
            gate,
        ],
        out_specs=[
            wide,
            edge,
            edge,
            gate,
            gate,
            pl.BlockSpec((taps + 4, 8, width), lambda j, s: (0, 0, j)),
        ],
        out_shape=[
            jax.ShapeDtypeStruct(branch.shape, BF),
            edge_shape,
            edge_shape,
            gate_shape,
            gate_shape,
            jax.ShapeDtypeStruct((taps + 4, 8, channels), F32),
        ],
        scratch_shapes=[
            pltpu.VMEM((length + 8, width), F32),
            pltpu.VMEM((length + 8, width), F32),
            pltpu.VMEM((length, width), F32),
            pltpu.VMEM((length, width), F32),
            pltpu.VMEM((length, width), BF),
            pltpu.VMEM((length, width), BF),
            pltpu.VMEM((length + 8, width), F32),
        ],
        cost_estimate=TINY,
        name="backward_gates",
    )(local_c, prod_c, carry_in, state, state_in, conv_out, branch, halo, conv_w, vectors, rate_w, inlet_w)


def outer_kernel(values, cotangent, out):
    out[...] = lax.dot_general(
        values[...], cotangent[...], (((0,), (0,)), ((), ())), preferred_element_type=F32
    ).astype(BF)


def run_outer(values, cotangent):
    values = values.reshape(-1, values.shape[-1])
    cotangent = cotangent.reshape(-1, cotangent.shape[-1])
    rows, channels = values.shape
    width = cotangent.shape[1]
    block = 256 if channels % 256 == 0 else channels
    return pl.pallas_call(
        outer_kernel,
        grid=(channels // block,),
        in_specs=[
            pl.BlockSpec((rows, block), lambda i: (0, i)),
            pl.BlockSpec((rows, width), lambda i: (0, 0)),
        ],
        out_specs=pl.BlockSpec((block, width), lambda i: (i, 0)),
        out_shape=jax.ShapeDtypeStruct((channels, width), BF),
        cost_estimate=TINY,
        name="outer",
    )(values, cotangent)


def two_products_kernel(first, first_w, second, second_w, out):
    total = jnp.dot(first[...], first_w[...], preferred_element_type=F32)
    total = total + jnp.dot(second[...], second_w[...], preferred_element_type=F32)
    out[...] = total.astype(BF)


def run_two_products(first, first_w, second, second_w):
    lead = first.shape[:-1]
    inner = first.shape[-1]
    first, second = first.reshape(-1, inner), second.reshape(-1, inner)
    rows, width = first.shape[0], first_w.shape[1]
    block = 256 if width % 256 == 0 else width
    whole = pl.BlockSpec((rows, inner), lambda i: (0, 0))
    column = pl.BlockSpec((inner, block), lambda i: (0, i))
    total = pl.pallas_call(
        two_products_kernel,
        grid=(width // block,),
        in_specs=[whole, column, whole, column],
        out_specs=pl.BlockSpec((rows, block), lambda i: (0, i)),
        out_shape=jax.ShapeDtypeStruct((rows, width), BF),
        cost_estimate=TINY,
        name="two_products",
    )(first, first_w, second, second_w)
    return total.reshape(*lead, width)


def norm_back_kernel(values, gain, mine, other, direct, total, rounded, sums):
    v = values[...]
    inv_rms = lax.rsqrt(jnp.mean(v * v, axis=-1, keepdims=True) + EPS)
    unit = v * inv_rms
    cot = mine[...].astype(F32) + other[...].astype(F32)
    scaled = cot * gain[...]
    grad = inv_rms * (scaled - unit * jnp.mean(scaled * unit, axis=-1, keepdims=True))
    found = direct[...] + grad
    total[...] = found
    rounded[...] = found.astype(BF)

    @pl.when(pl.program_id(0) == 0)
    def _():
        sums[...] = jnp.zeros_like(sums)

    part = cot * unit
    fold = part[0:8]
    for row in range(8, part.shape[0], 8):
        fold = fold + part[row : row + 8]
    sums[...] += fold


def run_norm_back(values, gain_vec, mine, other, direct):
    shape = values.shape
    width = shape[-1]
    values, mine, other, direct = (v.reshape(-1, width) for v in (values, mine, other, direct))
    rows = values.shape[0]
    block = 128
    some = pl.BlockSpec((block, width), lambda i: (i, 0))
    total, rounded, sums = pl.pallas_call(
        norm_back_kernel,
        grid=(rows // block,),
        in_specs=[some, pl.BlockSpec((1, width), lambda i: (0, 0)), some, some, some],
        out_specs=[some, some, pl.BlockSpec((8, width), lambda i: (0, 0))],
        out_shape=[
            jax.ShapeDtypeStruct(values.shape, F32),
            jax.ShapeDtypeStruct(values.shape, BF),
            jax.ShapeDtypeStruct((8, width), F32),
        ],
        cost_estimate=TINY,
        name="norm_back",
    )(values, gain_vec[None], mine, other, direct)
    return total.reshape(shape), rounded.reshape(shape), jnp.sum(sums, axis=0)


def rms_norm(values, gain_vec):
    inv_rms = lax.rsqrt(jnp.mean(values * values, axis=-1, keepdims=True) + EPS)
    return values * inv_rms * gain_vec


def norm_back(values, gain_vec, cot):
    inv_rms = lax.rsqrt(jnp.mean(values * values, axis=-1, keepdims=True) + EPS)
    unit = values * inv_rms
    scaled = cot * gain_vec
    grad = inv_rms * (scaled - unit * jnp.mean(scaled * unit, axis=-1, keepdims=True))
    return grad, jnp.sum(cot * unit, axis=(0, 1))


def times(values, matrix, dtype=F32):
    return jnp.einsum("slk,kn->sln", values, matrix, preferred_element_type=dtype)


def times_t(values, matrix, dtype=F32):
    return jnp.einsum("sln,kn->slk", values, matrix, preferred_element_type=dtype)


def outer_sum(values, cotangent):
    return jnp.einsum("slk,sln->kn", values, cotangent, preferred_element_type=F32).astype(BF)


def shards(
    inputs,
    teacher,
    seq_lengths,
    first_gain,
    branch_weight,
    branch_bias,
    gate_weight,
    gate_bias,
    conv_weight,
    conv_bias,
    rate_weight,
    rate_bias,
    inlet_weight,
    inlet_bias,
    decay_param,
    out_weight,
    second_gain,
    geglu_gate,
    geglu_up,
    geglu_down,
):
    seq_dev, local_len, model_width = inputs.shape
    tp = lax.axis_size("tp")
    fsdp = lax.axis_size("fsdp")
    chips = fsdp // 2
    full_len = local_len * tp
    me = lax.axis_index("fsdp")
    z = lax.axis_index("tp")
    core = me & 1
    chip = me // 2
    width = rate_weight.shape[2]
    taps = conv_weight.shape[0]

    bits = bits_of(chips)
    near, far = bits[: len(bits) // 2], bits[len(bits) // 2 :]
    every = list(range(chips))

    def block_order(some):
        held = [0]
        for bit in some:
            held = sorted(held + [j ^ bit for j in held])
        return held

    lanes = 2 * model_width // fsdp
    half_r = branch_weight.shape[1] // 2
    half_f = geglu_gate.shape[1] // 2

    def same_chip(values):
        return swap(values, "fsdp", 1)

    def both_rows(values):
        return in_core_order(values, same_chip(values), core, 0)

    def units(matrices):
        def half(which):
            parts = [pick_half(m, which, axis) for m, axis in matrices]
            return jnp.concatenate([p.T if a == 1 else p for p, (_, a) in zip(parts, matrices)], axis=0)

        return in_core_order(half(core), same_chip(half(1 - core)), core, 1)

    x4 = both_rows(inputs)
    lengths4 = both_rows(seq_lengths)
    count = jnp.broadcast_to(jnp.sum(lengths4.astype(F32)), (8, 128))
    for b in bits:
        count = count + swap(count, "fsdp", 2 * b)
    valid_total = count[0, 0]
    unit_r = units([(branch_weight, 1), (gate_weight, 1), (out_weight, 0)])
    unit_f = units([(geglu_gate, 1), (geglu_up, 1), (geglu_down, 0)])

    rows_chip = 2 * rate_weight.shape[1]
    pair_size = 2 * rows_chip * width
    pair_lines = -(-pair_size // (16 * lanes)) * 16
    pair = jnp.concatenate([rate_weight, inlet_weight], axis=1)
    unit_p = in_core_order(
        pick_half(pair, core, 0).reshape(2, -1, width),
        same_chip(pick_half(pair, 1 - core, 0)).reshape(2, -1, width),
        core,
        1,
    )
    unit_p = jnp.pad(unit_p.reshape(-1), (0, pair_lines * lanes - pair_size)).reshape(pair_lines, lanes)

    def all_z(values):
        return lax.all_gather(values, "tp", axis=0, tiled=False)

    def flat(values):
        return values.reshape(-1, values.shape[-1])

    top = tp // 2

    def rows_of(gathered, start, count, blocks=slice(None)):
        return flat(gathered[blocks, start : start + count])

    first_z = all_z(jnp.concatenate([unit_r[: 2 * half_r], unit_p], axis=0))
    second_z = all_z(after(unit_f[: 2 * half_f], first_z))
    out_own = unit_r[2 * half_r :]
    out_parts = {0: out_own} | {j: swap(out_own, "fsdp", 2 * j) for j in every[1:]}
    first_z, x4, lengths4, valid_total, out_parts = fence(first_z, x4, lengths4, valid_total, out_parts)
    a1 = jnp.concatenate([rows_of(first_z, 0, half_r), rows_of(first_z, 2 * half_r, pair_lines)], axis=0)
    b1 = rows_of(first_z, half_r, half_r)
    left_a, left_b = block_order(near), block_order(far)
    a1, b1 = spread({0: a1}, near), spread({0: b1}, far)
    first_a, first_b = a1[near[-1]], b1[far[-1]]
    a1, b1 = spread(a1, far), spread(b1, near)
    a3, b3 = {0: rows_of(second_z, 0, half_f)}, {0: rows_of(second_z, half_f, half_f)}
    local_vectors = jnp.concatenate(
        [
            conv_weight,
            jnp.stack([branch_bias, gate_bias, conv_bias, rate_bias, inlet_bias, decay_param]),
        ],
        axis=0,
    )
    held = pick_half(after(local_vectors, first_a, first_b), core, 1)
    for b in bits_of(tp):
        held = jnp.concatenate([held, swap(held, "tp", b)], axis=1)
    held = xor_blocks(held, 1, tp, z)

    def to_chip(values):
        return xor_blocks(values, values.ndim - 1, chips, chip)

    gain1, gain2 = to_chip(first_gain), to_chip(second_gain)
    x4 = to_chip(x4)
    residual = x4.astype(F32)
    first_rows = rms_norm(residual, gain1).astype(BF)
    a1, b1, a3, b3, held, first_rows = fence(a1, b1, a3, b3, held, first_rows)
    out_z = all_z(after(join(out_parts), second_z, a1[0]))
    third_z = all_z(after(unit_f[2 * half_f :], out_z))
    a3, b3 = spread(a3, near), spread(b3, far)
    far_a = {k ^ j: swap(a3[k], "fsdp", 2 * j) for k in [0] for j in far[:1]}
    near_b = {k ^ j: swap(b3[k], "fsdp", 2 * j) for k in [0] for j in near[:1]}
    size_r = tp * half_r
    w_branch, w_gate = join(a1, 0, size_r), join(b1, 0, size_r)
    w_out = flat(out_z)
    w_pair = [a1[j][size_r : size_r + tp * pair_lines].reshape(tp, -1)[:, :pair_size] for j in every]
    w_pair = jnp.stack(w_pair, axis=1).reshape(tp, chips, 2, rows_chip, width)
    w_pair = xor_blocks(w_pair, 1, chips, chip).transpose(2, 0, 1, 3, 4).reshape(2, tp, chips * rows_chip, width)
    w_rate, w_inlet = w_pair[0], w_pair[1]

    taps_w = held[:taps]
    b_branch, b_gate, b_conv, b_rate, b_inlet, decay_vec = (held[taps + k] for k in range(6))
    soft = jax.nn.softplus(-decay_vec)
    vectors = jnp.stack([b_conv, b_rate, b_inlet, soft])

    branch_pre = times_t(first_rows, w_branch) + b_branch

    def along_z(values, shift):
        return lax.ppermute(values, "tp", [(i, i + shift) for i in range(tp) if 0 <= i + shift < tp])

    halo = jnp.pad(along_z(branch_pre[:, local_len - taps + 1 :], 1), ((0, 0), (8 - taps + 1, 0), (0, 0)))
    conv_out, decay_rate, local_state, prod_decay = run_forward(
        branch_pre, halo, taps_w, vectors, w_rate, w_inlet
    )
    ends = jnp.stack([prod_decay[:, -1], local_state[:, -1]])
    state_in = jnp.zeros_like(ends[0])
    for shift in reversed(range(1, tp)):
        got = along_z(ends, shift)
        state_in = got[1] + got[0] * state_in
    state_in = state_in[:, None]
    state_in, a3, b3, far_a, near_b = fence(state_in, a3, b3, far_a, near_b)
    gate_pre = times_t(after(first_rows, state_in), w_gate) + b_gate
    a3, b3 = finish(a3, far_a, far), finish(b3, near_b, near)
    state = local_state + prod_decay * state_in
    mixed = (state * jax.nn.gelu(gate_pre)).astype(BF)
    def core_sum(term):
        return term.astype(F32) + same_chip(term).astype(F32)

    out_term, a3, b3, third_z = fence(times(mixed, w_out, BF), a3, b3, third_z)
    a4, b4 = {0: flat(third_z[:top])}, {0: flat(third_z[top:])}
    a4, b4 = spread(a4, near), spread(b4, far)
    w_ffgate, w_ffup = join(a3), join(b3)
    middle = residual + core_sum(out_term)
    second_rows = rms_norm(middle, gain2).astype(BF)
    second_rows, a4, b4 = fence(second_rows, a4, b4)
    a4, b4 = spread(a4, far), spread(b4, near)
    teacher4 = both_rows(after(teacher, second_rows))
    ff_gate = times_t(second_rows, w_ffgate)
    ff_up = times_t(second_rows, w_ffup)
    ff_hidden = (jax.nn.gelu(ff_gate) * ff_up).astype(BF)
    ff_hidden, a4, b4, teacher4 = fence(ff_hidden, a4, b4, teacher4)
    w_ffdown = join(a4, 0, None, b4, 0)
    final = middle + core_sum(times(ff_hidden, w_ffdown, BF))

    positions = z * local_len + jnp.arange(local_len, dtype=jnp.int32)
    valid_mask = (positions[None, :] < lengths4[:, None]).astype(F32)[..., None]
    teacher4 = to_chip(teacher4).astype(F32)
    mismatch = final - teacher4
    loss_part = jnp.sum(valid_mask * mismatch * mismatch)
    scaling = seq_dev * fsdp * full_len / valid_total
    out_cot = valid_mask * mismatch * scaling
    ff_cot = out_cot.astype(BF)

    def by_z(a, b):
        return lax.psum_scatter(
            jnp.concatenate([a.reshape(tp, -1, lanes), b.reshape(tp, -1, lanes)], axis=1),
            "tp",
            scatter_dimension=0,
            tiled=False,
        )

    def halves(grad):
        return jnp.split(grad, 2, axis=0)

    def far_first(grad):
        return shrink(grad, every, far)[0]

    def near_first(grad):
        return shrink(grad, every, near)[0]

    def far_last(grad):
        return shrink(grad, left_b, far)[0]

    def near_last(grad):
        return shrink(grad, left_a, near)[0]

    ff_cot, g_ffdown = fence(ff_cot, outer_sum(ff_hidden, ff_cot))
    down_sum = lax.psum_scatter(g_ffdown.reshape(tp, half_f, model_width), "tp", scatter_dimension=0, tiled=False)
    d_hidden = times_t(ff_cot, w_ffdown)
    act, slope = gelu_parts(ff_gate)
    d_up = (d_hidden * act).astype(BF)
    d_ffgate = (d_hidden * ff_up * slope).astype(BF)
    g_ffgate = run_outer(d_ffgate, second_rows)
    d_ffgate, d_up, g_ffgate = fence(d_ffgate, d_up, g_ffgate)
    top_g, low_g = halves(g_ffgate)
    a3, b3 = far_first(top_g), near_first(low_g)
    g_ffup = run_outer(d_up, second_rows)
    d_second = run_two_products(d_ffgate, w_ffgate, after(d_up, g_ffup), w_ffup)
    d_second, a3, b3, g_ffup = fence(d_second, a3, b3, g_ffup)
    top_u, low_u = halves(g_ffup)
    a6, b6 = far_first(top_u), near_first(low_u)
    d_middle, mid_cot, g_second = run_norm_back(middle, gain2, d_second, same_chip(d_second), out_cot)
    mid_cot, a3, b3 = fence(mid_cot, a3, b3)
    a3, b3 = near_last(a3), far_last(b3)
    d_mixed = times_t(mid_cot, w_out)
    d_gate, local_c, prod_c = run_backward_scan(d_mixed, gate_pre, state, decay_rate, width)
    d_gate, local_c, prod_c, a3, b3, a6, b6, down_sum = fence(d_gate, local_c, prod_c, a3, b3, a6, b6, down_sum)
    a6, b6 = near_last(a6), far_last(b6)
    top_d, low_d = halves(down_sum)
    a4, b4 = far_first(top_d), near_first(low_d)
    starts = jnp.stack([prod_c[:, 0], local_c[:, 0]]) * decay_rate[:, 0]
    carry_in = jnp.zeros_like(starts[0])
    for shift in reversed(range(1, tp)):
        got = along_z(starts, -shift)
        carry_in = got[1] + got[0] * carry_in
    g_out = outer_sum(after(mixed, d_gate), mid_cot)
    g_gate = outer_sum(d_gate, first_rows)
    local_c, g_gate, g_out, a4, b4, a6, b6 = fence(local_c, g_gate, g_out, a4, b4, a6, b6)
    gate_sum = jnp.concatenate([a3, b3], axis=0).reshape(tp, -1, lanes)
    up_sum = jnp.concatenate([a6, b6], axis=0).reshape(tp, -1, lanes)
    unit_gu = jnp.concatenate([gate_sum, up_sum], axis=1)
    unit_gu = lax.psum_scatter(unit_gu, "tp", scatter_dimension=0, tiled=False)
    a4, b4 = near_last(a4), far_last(b4)
    a2, b1 = far_first(g_out), near_first(g_gate)
    d_branch, head, tail, g_rate, g_inlet, sums = run_backward_gates(
        local_c,
        prod_c,
        carry_in[:, None],
        state,
        state_in,
        conv_out,
        branch_pre,
        halo,
        taps_w,
        vectors,
        w_rate,
        w_inlet,
    )
    d_branch, head, a2, b1, a4, b4 = fence(d_branch, head, a2, b1, a4, b4)
    unit_d = jnp.concatenate([a4, b4], axis=0)
    ahead = along_z(head[:, : taps - 1], -1)
    edge = tail[:, 8 - taps + 1 :]
    for k in range(1, taps):
        first = taps - 1 - k
        edge = edge.at[:, first:].add(taps_w[k] * ahead[:, :k])
    d_branch = lax.dynamic_update_slice(d_branch, edge.astype(BF), (0, local_len - taps + 1, 0))

    a2, b1 = near_last(a2), far_last(b1)
    g_branch = outer_sum(d_branch, first_rows)
    g_rate, g_inlet, d_branch, a2, b1, g_branch, unit_gu = fence(
        g_rate, g_inlet, d_branch, a2, b1, g_branch, unit_gu
    )
    unit_og = by_z(a2, b1)
    top_b, low_b = halves(g_branch)
    a1, b5 = far_first(top_b), near_first(low_b)
    g_pair = jnp.stack([g_rate, g_inlet]).reshape(2, tp, chips, rows_chip, width)
    g_pair = xor_blocks(g_pair, 2, chips, chip).astype(BF).transpose(1, 2, 0, 3, 4).reshape(tp, chips, -1)
    g_pair = jnp.pad(g_pair, ((0, 0), (0, 0), (0, pair_lines * lanes - pair_size)))
    g_pair = g_pair.reshape(tp, chips, pair_lines, lanes).transpose(0, 2, 1, 3).reshape(-1, model_width)
    g_pair, a1, b5, d_branch = fence(g_pair, a1, b5, d_branch)
    top_p, low_p = halves(g_pair)
    ap, bp = far_first(top_p), near_first(low_p)
    a1, b5 = near_last(a1), far_last(b5)
    d_first_part = (times(d_branch, w_branch) + times(d_gate, w_gate)).astype(BF)
    d_first_part, a1, b5, ap, bp, unit_og = fence(d_first_part, a1, b5, ap, bp, unit_og)
    ap, bp = near_last(ap), far_last(bp)
    unit_b = [jnp.concatenate(v, axis=0).reshape(tp, -1, lanes) for v in ((a1, b5), (ap, bp))]
    unit_b = lax.psum_scatter(jnp.concatenate(unit_b, axis=1), "tp", scatter_dimension=0, tiled=False)

    def own(values):
        return pick_half(values, core, 0)

    d_first = own(d_first_part).astype(F32) + same_chip(pick_half(d_first_part, 1 - core, 0)).astype(F32)
    d_in_norm, g_first = norm_back(own(residual), gain1, d_first)
    input_grad = to_chip(own(d_middle) + d_in_norm)
    block_out = to_chip(own(final).astype(BF))

    def to_own(grad, channel_axis):
        mine = pick_half(grad, core, 1)
        other = same_chip(pick_half(grad, 1 - core, 1))
        whole = in_core_order(mine, other, core, 0)
        return (whole.T if channel_axis == 1 else whole).astype(F32)

    pair_g = unit_b[half_r:].reshape(-1)[:pair_size].reshape(2, rows_chip, width)
    pair_g = in_core_order(
        pick_half(pair_g, core, 1)[None], same_chip(pick_half(pair_g, 1 - core, 1))[None], core, 0
    ).astype(F32)

    sums = jnp.sum(sums, axis=1)
    small = jnp.concatenate(
        [
            jnp.stack(
                [
                    jnp.sum(d_branch.astype(F32), axis=(0, 1)),
                    jnp.sum(d_gate.astype(F32), axis=(0, 1)),
                    sums[0] * (DECAY_SCALE * jax.nn.sigmoid(-decay_vec)),
                ]
            ),
            sums[1:],
        ],
        axis=0,
    )
    found = jnp.concatenate(
        [
            to_chip(g_first),
            to_chip(0.5 * g_second),
            jnp.broadcast_to(0.5 * loss_part, (128,)),
            small.reshape(-1),
        ]
    ).reshape(-1, 128)
    for b in bits:
        found = found + swap(found, "fsdp", 2 * b)
    for b in bits_of(tp):
        found = found + swap(found, "tp", b)
    other = same_chip(found)
    lines = (2 * model_width + 128) // 128
    stats = (found[:lines] + other[:lines]).reshape(-1)
    block = lambda v: lax.dynamic_index_in_dim(v[lines:].reshape(small.shape[0], tp, half_r), z, 1, keepdims=False)
    small = in_core_order(block(found), block(other), core, 1)
    loss_value = stats[2 * model_width] / (model_width * valid_total)
    return (
        block_out,
        loss_value,
        input_grad,
        stats[:model_width],
        to_own(unit_b[:half_r], 1),
        small[0],
        to_own(unit_og[half_r:], 1),
        small[1],
        small[6:],
        small[5],
        pair_g[:, 0],
        small[3],
        pair_g[:, 1],
        small[4],
        small[2],
        to_own(unit_og[:half_r], 0),
        stats[model_width : 2 * model_width],
        to_own(unit_gu[:half_f], 1),
        to_own(unit_gu[half_f:], 1),
        to_own(unit_d, 0),
    )


def solution(mesh):
    rows = P("fsdp", "tp", None)
    by_column, by_row = P("fsdp", "tp"), P("tp", "fsdp")
    blocks = P("tp", "fsdp", None)
    channel = P("tp")
    return jax.shard_map(
        shards,
        mesh=mesh,
        in_specs=(
            rows,
            rows,
            P("fsdp"),
            P(),
            by_column,
            channel,
            by_column,
            channel,
            P(None, "tp"),
            channel,
            blocks,
            channel,
            blocks,
            channel,
            channel,
            by_row,
            P(),
            by_column,
            by_column,
            by_row,
        ),
        out_specs=(
            rows,
            P(),
            rows,
            P(),
            by_column,
            channel,
            by_column,
            channel,
            P(None, "tp"),
            channel,
            blocks,
            channel,
            blocks,
            channel,
            channel,
            by_row,
            P(),
            by_column,
            by_column,
            by_row,
        ),
        check_vma=False,
    )
```
